256 devices in a mesh: dp: 16 (over x, z_hi, core), seq: 16 (over z_lo, y).
Axes of the slice: x: 4, y: 4, z: 8 (z_hi: 2, z_lo: 4; z = z_hi * 4 + z_lo), core: 2. Of those that a mesh axis runs over, the one named last changes fastest.
Arguments:
- tokens: bfloat16 [32, 2304, 1280], P('dp', 'seq'), may hold values from -60 to 60
- pre_gain: float32 [1280], replicated, may hold values from 0.5 to 1.5
- pre_shift: float32 [1280], replicated, may hold values from -3 to 3
- w_qkv: bfloat16 [1280, 3840], P('dp'), may hold values from -4 to 4
- qkv_bias: float32 [3840], replicated, may hold values from -3 to 3
- w_out: bfloat16 [1280, 1280], P('dp'), may hold values from -0.15625 to 0.15625
- out_bias: float32 [1280], replicated, may hold values from -3 to 3
- mlp_gain: float32 [1280], replicated, may hold values from 0.5 to 1.5
- mlp_shift: float32 [1280], replicated, may hold values from -3 to 3
- w_up: bfloat16 [1280, 2560], P('dp'), may hold values from -0.15625 to 0.15625
- up_bias: float32 [2560], replicated, may hold values from -3 to 3
- w_down: bfloat16 [2560, 1280], P('dp'), may hold values from -0.125 to 0.125
- down_bias: float32 [1280], replicated, may hold values from -3 to 3
Outputs:
- layer_out: bfloat16 [32, 2304, 1280], P('dp', 'seq')
The draws below stay inside these ranges and needn't reach their ends.
All inputs are finite; a program needn't handle non-finite values.
Results may differ from the reference program's by a relative error of at most 0.0039.
Values may be sent and summed in bfloat16 or wider, within the bound.
A program may use at most 128 MiB of HBM per device.

```python
import math
import jax
import jax.numpy as jnp
from jax import lax

D = 1280
HEADS = 16
HEAD_DIM = 80
FF = 2560
IMAGES = 32
SEQ_LEN = 2304


def draw_tokens(key, part):
    subkeys = jax.random.split(jax.random.fold_in(key, 21), 4)
    shape = (IMAGES, SEQ_LEN, D)
    base = jax.random.normal(subkeys[0], shape, jnp.float32)
    row_scale = jnp.exp(jax.random.uniform(subkeys[2], (IMAGES, SEQ_LEN, 1), jnp.float32, math.log(0.4), math.log(4.0)))
    col_scale = jnp.exp(jax.random.uniform(subkeys[3], (1, 1, D), jnp.float32, math.log(0.4), math.log(4.0)))
    values = base * row_scale * col_scale
    return jnp.clip(values, -60.0, 60.0).astype(jnp.bfloat16)


def draw_w_qkv(key, part):
    subkey = jax.random.fold_in(key, 33)
    shape = (D, 3 * D)
    values = jnp.clip(jax.random.normal(subkey, shape, jnp.float32), -6.0, 6.0) / math.sqrt(D)
    return values.astype(jnp.bfloat16)


def block_levels(stream_key, extent, cuts, smallest, top_value):
    def one(axis_at, blocks):
        steps = jax.random.uniform(jax.random.fold_in(jax.random.fold_in(stream_key, 6), axis_at), (blocks,), jnp.float32, smallest / len(cuts), top_value / len(cuts))
        return jnp.repeat(jnp.exp(steps), extent[axis_at] // blocks).reshape((-1,) + (1,) * (len(extent) - axis_at - 1))

    level = one(*cuts[0])
    for cut in cuts[1:]:
        level = level * one(*cut)
    return level


def bell_draw(stream_key, extent, deviation, bound, cuts=(), held_as=jnp.bfloat16):
    array = jax.random.normal(stream_key, extent, jnp.float32) * deviation
    if len(cuts) > 0:
        array = block_levels(stream_key, extent, cuts, -0.22, 0.18) * array
    return jnp.clip(array, min=-bound, max=bound).astype(held_as)


def setup_inputs(seed: int = 0) -> dict:
    key_of = jax.random.split(jax.random.key(seed), 14)
    return {
        "tokens": draw_tokens(jax.random.fold_in(key_of[13], 71), 0),
        "pre_gain": jnp.clip(1.0 + 0.1 * jax.random.normal(key_of[1], (D,), jnp.float32), 0.5, 1.5),
        "pre_shift": bell_draw(key_of[2], (D,), 0.5, 3.0, (), jnp.float32),
        "w_qkv": draw_w_qkv(jax.random.fold_in(key_of[13], 71), 0),
        "qkv_bias": bell_draw(key_of[4], (3 * D,), 0.5, 3.0, (), jnp.float32),
        "w_out": bell_draw(key_of[5], (D, D), D ** -0.5, 0.15625, ((0, 16),)),
        "out_bias": bell_draw(key_of[6], (D,), 0.5, 3.0, (), jnp.float32),
        "mlp_gain": jnp.clip(1.0 + 0.1 * jax.random.normal(key_of[7], (D,), jnp.float32), 0.5, 1.5),
        "mlp_shift": bell_draw(key_of[8], (D,), 0.5, 3.0, (), jnp.float32),
        "w_up": bell_draw(key_of[9], (D, FF), D ** -0.5, 0.15625, ((0, 16),)),
        "up_bias": bell_draw(key_of[10], (FF,), 0.5, 3.0, (), jnp.float32),
        "w_down": bell_draw(key_of[11], (FF, D), FF ** -0.5, 0.125, ((0, 16),)),
        "down_bias": bell_draw(key_of[12], (D,), 0.5, 3.0, (), jnp.float32),
    }


EPSILON = 1e-05

def normalize(features, gain, shift):
    average = lax.optimization_barrier(jnp.mean(features, axis=-1, keepdims=True))
    centered = features - average
    spread = lax.optimization_barrier(jnp.mean(centered * centered, axis=-1, keepdims=True))
    return centered * lax.rsqrt(spread + EPSILON) * gain + shift

def attend_head(packed_head):
    queries = packed_head[:, :HEAD_DIM]
    key_rows = packed_head[:, HEAD_DIM:2 * HEAD_DIM]
    value_rows = packed_head[:, 2 * HEAD_DIM:]
    scores = jnp.dot(queries, key_rows.T, preferred_element_type=jnp.float32) * (1.0 / math.sqrt(HEAD_DIM))
    highest = lax.optimization_barrier(jnp.max(scores, axis=-1, keepdims=True))
    weights = jnp.exp(scores - highest)
    probs = (weights / lax.optimization_barrier(jnp.sum(weights, axis=-1, keepdims=True))).astype(jnp.bfloat16)
    return jnp.dot(probs, value_rows, preferred_element_type=jnp.float32).astype(jnp.bfloat16)

def reference(tokens, pre_gain, pre_shift, w_qkv, qkv_bias, w_out, out_bias, mlp_gain, mlp_shift, w_up, up_bias, w_down, down_bias):

    def one_picture(picture):
        residual = picture.astype(jnp.float32)
        normed = normalize(residual, pre_gain, pre_shift).astype(jnp.bfloat16)
        packed = (jnp.dot(normed, w_qkv, preferred_element_type=jnp.float32) + qkv_bias).astype(jnp.bfloat16)
        per_head = packed.reshape(SEQ_LEN, HEADS, 3 * HEAD_DIM).transpose(1, 0, 2)
        context = lax.map(attend_head, per_head)
        context = context.transpose(1, 0, 2).reshape(SEQ_LEN, D)
        middle = residual + jnp.dot(context, w_out, preferred_element_type=jnp.float32) + out_bias
        normed_mlp = normalize(middle, mlp_gain, mlp_shift).astype(jnp.bfloat16)
        lifted = jnp.dot(normed_mlp, w_up, preferred_element_type=jnp.float32) + up_bias
        hidden = jax.nn.gelu(lifted, approximate=False).astype(jnp.bfloat16)
        lowered = jnp.dot(hidden, w_down, preferred_element_type=jnp.float32)
        return (middle + lowered + down_bias).astype(jnp.bfloat16)
    return lax.map(one_picture, tokens)
```

```python
import math

import jax
import jax.numpy as jnp
from jax import lax
from jax.experimental import pallas as pl
from jax.experimental.pallas import tpu as pltpu
from jax.sharding import PartitionSpec as P

D = 1280
HEADS = 16
HEAD_DIM = 80
FF = 2560
TOK = 144
SEQ = 2304
HALF = 1920
PAIR = 480
EPSILON = 1e-05
EXP_SCALE = math.log2(math.e) / math.sqrt(HEAD_DIM)

MESH = pl.DeviceIdType.MESH
F32 = jnp.float32
BF16 = jnp.bfloat16

COLS = (HALF, D, FF, D)
LOW = (1024, 640, 1280, 640)
ROWS = (80, 80, 80, 160)
XM, XP, X2L, X2R, ZC, YC, DC = 0, 1, 2, 3, 8, 9, 10


def kernel(
    x_ref, pre_gain, pre_shift, qkv_bias, out_bias, mlp_gain, mlp_shift, up_bias, down_bias,
    wqkv_in, wout_in, wup_in, wdown_in,
    o_ref,
    wqkv, wout, wup, wdown,
    tok, other, packed, qsend, qin, qb, kb, vb, csend, cin, zsend, ctx, mid, normed_mlp, hid,
    load_sem, w_send, w_recv, t_send, t_recv, y_send, y_recv, c_send, c_recv, z_send, z_recv,
):
    dp = lax.axis_index("dp")
    sq = lax.axis_index("seq")
    x, zh, c = dp // 4, (dp // 2) % 2, dp % 2
    zl, y = sq // 4, sq % 4
    half, part = zl // 2, zl % 2

    def dev(x=x, zh=zh, c=c, zl=zl, y=y):
        return ((x * 2 + zh) * 2 + c, zl * 4 + y)

    xr, xl, xo = (x + 1) % 4, (x + 3) % 4, (x + 2) % 4
    ypair = y + 1 - 2 * (y % 2)
    partner = zl + 1 - 2 * part
    near_here = 1 + half
    is_near = zl == near_here
    near_other = 2 - half
    far_other = 3 - 3 * half

    barrier = pltpu.get_barrier_semaphore()
    peers = [dev(x=xr), dev(x=xl), dev(zh=1 - zh), dev(c=1 - c)]
    peers += [dev(zl=(zl + d) % 4) for d in (1, 2, 3)]
    peers += [dev(y=(y + d) % 4) for d in (1, 2, 3)]

    bufs = (wqkv, wout, wup, wdown)
    sources = (
        wqkv_in.at[:, pl.ds(pl.multiple_of(part * HALF, 128), HALF)],
        wout_in,
        wup_in,
        wdown_in,
    )
    loads = [
        pltpu.make_async_copy(sources[i], bufs[i].at[x, zh, c], load_sem.at[i]) for i in range(4)
    ]
    for load in loads:
        load.start()
    for peer in peers:
        pl.semaphore_signal(barrier, inc=1, device_id=peer, device_id_type=MESH)
    pl.semaphore_wait(barrier, len(peers))

    started = []

    def region(i, xx, zz, cc, lo=0, size=None):
        size = COLS[i] if size is None else size
        return bufs[i].at[xx, zz, cc, :, pl.ds(lo, size)]

    def w_copy(i, j, ref, target):
        return pltpu.make_async_remote_copy(
            src_ref=ref, dst_ref=ref, send_sem=w_send.at[i, j], recv_sem=w_recv.at[i, j],
            device_id=target, device_id_type=MESH,
        )

    def w_start(i, j, ref, target):
        copy = w_copy(i, j, ref, target)
        copy.start()
        started.append(copy)

    def w_wait(i, j, ref):
        w_copy(i, j, ref, dev(c=1 - c)).wait_recv()

    def side(k):
        return zh if k == 0 else 1 - zh

    def ring_start(i, k):
        mine = region(i, x, side(k), c)
        w_start(i, 4 * k + XM, mine, dev(x=xr))
        w_start(i, 4 * k + XP, mine, dev(x=xl))

    def ring_relay(i, k):
        low, high = LOW[i], COLS[i] - LOW[i]
        w_wait(i, 4 * k + XM, region(i, xl, side(k), c))
        w_start(i, 4 * k + X2L, region(i, xl, side(k), c, 0, low), dev(x=xr))
        w_wait(i, 4 * k + XP, region(i, xr, side(k), c))
        w_start(i, 4 * k + X2R, region(i, xr, side(k), c, low, high), dev(x=xl))

    def ring_end(i, k):
        low, high = LOW[i], COLS[i] - LOW[i]
        w_wait(i, 4 * k + X2L, region(i, xo, side(k), c, 0, low))
        w_wait(i, 4 * k + X2R, region(i, xo, side(k), c, low, high))
        w_start(i, DC + k, bufs[i].at[:, side(k), c], dev(c=1 - c))

    def sibling_wait(i, k):
        w_wait(i, DC + k, bufs[i].at[:, side(k), 1 - c])

    def cut(i, which):
        size = LOW[i]
        return pl.multiple_of(which * size, 128), size

    def class_start(i):
        if i == 0:
            w_start(i, ZC, region(i, x, zh, c), dev(zh=1 - zh))
        else:
            lo, size = cut(i, y % 2)
            w_start(i, ZC, region(i, x, zh, c, lo, size), dev(zh=1 - zh))

    def class_swap(i):
        lo, size = cut(i, y % 2)
        w_wait(i, ZC, region(i, x, 1 - zh, c, lo, size))
        w_start(i, YC, region(i, x, 1 - zh, c, lo, size), dev(y=ypair))

    def class_ring(i):
        if i == 0:
            w_wait(i, ZC, region(i, x, 1 - zh, c))
        else:
            lo, size = cut(i, 1 - y % 2)
            w_wait(i, YC, region(i, x, 1 - zh, c, lo, size))
        ring_start(i, 1)

    loads[0].wait()
    class_start(0)
    ring_start(0, 0)

    def norm_rows(rows, gain, shift):
        average = jnp.mean(rows, axis=-1, keepdims=True)
        centered = rows - average
        spread = jnp.mean(centered * centered, axis=-1, keepdims=True)
        return centered * lax.rsqrt(spread + EPSILON) * gain[...] + shift[...]

    def norm_image(image, store):
        @pl.loop(0, TOK // 16)
        def _(n):
            at = pl.ds(pl.multiple_of(n * 16, 16), 16)
            rows = x_ref[image, at, :].astype(F32)
            store(at, norm_rows(rows, pre_gain, pre_shift).astype(BF16))

    def store_other(at, value):
        other[at, :] = value

    def store_own(at, value):
        tok[zl, at, :] = value

    def t_copy(src, slot, j, target):
        return pltpu.make_async_remote_copy(
            src_ref=src, dst_ref=tok.at[slot], send_sem=t_send.at[j], recv_sem=t_recv.at[slot],
            device_id=target, device_id_type=MESH,
        )

    norm_image(1 - half, store_other)
    to_near = t_copy(other, zl, 1, dev(zl=near_other))
    to_near.start()
    to_far = t_copy(other, zl, 2, dev(zl=far_other))

    @pl.when(is_near)
    def _():
        to_far.start()

    norm_image(half, store_own)
    to_partner = t_copy(tok.at[zl], zl, 0, dev(zl=partner))
    to_partner.start()

    for load in loads[1:]:
        load.wait()

    class_ring(0)
    ring_relay(0, 0)
    for i in (1, 2, 3):
        ring_start(i, 0)
    onward = t_copy(tok.at[far_other], far_other, 3, dev(zl=partner))

    def token_wait(slot):
        t_copy(tok.at[slot], slot, 0, dev(zl=partner)).wait_recv()

    ring_end(0, 0)
    ring_relay(0, 1)

    @pl.when(is_near)
    def _():
        token_wait(far_other)
        onward.start()

    ring_end(0, 1)
    sibling_wait(0, 0)
    sibling_wait(0, 1)

    def slot_of(j):
        last = jnp.where(j == 2, near_other, far_other)
        return jnp.where(j == 0, zl, jnp.where(j == 1, partner, last))

    def y_copy(r, slot):
        to = (y + r) % 4
        return pltpu.make_async_remote_copy(
            src_ref=qsend.at[to, slot], dst_ref=qin.at[y, slot],
            send_sem=y_send.at[r - 1, slot], recv_sem=y_recv.at[r - 1, slot],
            device_id=dev(y=to), device_id_type=MESH,
        )

    @pl.loop(0, 4)
    def _(j):
        slot = slot_of(j)

        @pl.when((j > 0) & jnp.logical_not((j == 3) & is_near))
        def _():
            token_wait(slot)

        rows = tok[slot]
        for n in range(3):
            at = slice(640 * n, 640 * n + 640)
            block = wqkv[:, :, :, :, at].reshape(D, 640)
            packed[:, at] = jnp.dot(rows, block, preferred_element_type=F32) + qkv_bias[part, :, at]
        for to in range(4):
            start = PAIR * to // 128 * 128
            wide = packed[:, start : min(start + 640, HALF)]
            shift = PAIR * to - start
            if shift:
                wide = pltpu.roll(wide, wide.shape[1] - shift, 1)
            qsend[to, slot] = wide[:, :512].astype(BF16)
        qin[y, slot] = qsend[y, slot]
        for r in (2, 1, 3):
            y_copy(r, slot).start()

    for i in (1, 2, 3):
        class_start(i)
        ring_relay(i, 0)

    def y_copy_in(r, slot, source):
        return pltpu.make_async_remote_copy(
            src_ref=qin.at[source, slot], dst_ref=qin.at[source, slot],
            send_sem=y_send.at[r - 1, slot], recv_sem=y_recv.at[r - 1, slot],
            device_id=dev(y=(y + 1) % 4), device_id_type=MESH,
        )

    lane128 = lax.broadcasted_iota(jnp.int32, (TOK, 128), 1)
    lane256 = lax.broadcasted_iota(jnp.int32, (TOK, 256), 1)

    @pl.loop(0, 16)
    def _(n):
        j, r = n // 4, n % 4
        slot = slot_of(j)
        source = (y + 4 - r) % 4

        @pl.when(r > 0)
        def _():
            y_copy_in(r, slot, source).wait_recv()

        wide = qin[source, slot].astype(F32)
        at = pl.ds(pl.multiple_of((source * 4 + slot) * TOK, 16), TOK)
        keep = lane128 < HEAD_DIM
        k0 = pltpu.roll(wide, 512 - 80, 1)
        v0 = pltpu.roll(wide, 512 - 160, 1)
        q1 = pltpu.roll(wide, 512 - 240, 1)
        k1 = pltpu.roll(wide, 512 - 320, 1)
        qb[0, at, :] = jnp.where(keep, wide[:, :128], 0.0).astype(BF16)
        qb[1, at, :] = jnp.where(keep, q1[:, :128], 0.0).astype(BF16)
        kb[0, at, :] = jnp.where(keep, k0[:, :128], 0.0).astype(BF16)
        kb[1, at, :] = jnp.where(keep, k1[:, :128], 0.0).astype(BF16)
        ones = jnp.where(lane256 == 160, 1.0, 0.0)
        vb[0, at, :] = jnp.where(lane256 < 80, v0[:, :256], ones).astype(BF16)
        in_second = (lane256 >= 80) & (lane256 < 160)
        vb[1, at, :] = jnp.where(in_second, k1[:, :256], ones).astype(BF16)

    for i in (1, 2, 3):
        ring_end(i, 0)
    for i in (1, 2, 3):
        class_swap(i)

    def c_copy(t, r):
        to = (y + r) % 4
        return pltpu.make_async_remote_copy(
            src_ref=csend.at[to], dst_ref=cin.at[y],
            send_sem=c_send.at[t], recv_sem=c_recv.at[t],
            device_id=dev(y=to), device_id_type=MESH,
        )

    def c_wait(t, r):
        source = (y + 4 - r) % 4
        pltpu.make_async_remote_copy(
            src_ref=cin.at[source], dst_ref=cin.at[source],
            send_sem=c_send.at[t], recv_sem=c_recv.at[t],
            device_id=dev(y=(y + 1) % 4), device_id_type=MESH,
        ).wait_recv()

    def attend(to, n):
        at = pl.ds(pl.multiple_of((to * 4 + n) * TOK, 16), TOK)
        sums = []
        for head in range(2):
            scores = lax.dot_general(
                qb[head, at, :], kb[head], (((1,), (1,)), ((), ())), preferred_element_type=F32
            )
            highest = jnp.max(scores, axis=-1, keepdims=True) * EXP_SCALE
            weights = jnp.exp2(scores * EXP_SCALE - highest).astype(BF16)
            total = jnp.dot(weights, vb[head], preferred_element_type=F32)
            sums.append(total / total[:, 160:161])
        mixed = jnp.where(lane256 < 80, sums[0], jnp.where(lane256 < 160, sums[1], 0.0))
        csend[to, pl.ds(pl.multiple_of(n * TOK, 16), TOK), :] = mixed.astype(BF16)

    order = (2, 1, 3, 0)
    for t, r in enumerate(order):
        to = (y + r) % 4

        @pl.loop(0, 4)
        def _(n):
            attend(to, n)

        if r:
            c_copy(t, r).start()
        if t == 0:
            for i in (1, 2, 3):
                class_ring(i)
        if t == 2:
            ring_relay(1, 1)
        if t == 3:
            ring_relay(2, 1)

    cin[y] = csend[y]
    for t, r in enumerate(order[:3]):
        c_wait(t, r)

    def z_copy(d):
        to = (zl + d) % 4
        return pltpu.make_async_remote_copy(
            src_ref=zsend.at[d],
            dst_ref=ctx.at[half, :, pl.ds(pl.multiple_of(640 * part, 128), 640)],
            send_sem=z_send.at[d], recv_sem=z_recv.at[d],
            device_id=dev(zl=to), device_id_type=MESH,
        )

    def z_wait(d):
        source = (zl + 4 - d) % 4
        ref = ctx.at[source // 2, :, pl.ds(pl.multiple_of(640 * (source % 2), 128), 640)]
        pltpu.make_async_remote_copy(
            src_ref=ref, dst_ref=ref, send_sem=z_send.at[d], recv_sem=z_recv.at[d],
            device_id=dev(zl=partner), device_id_type=MESH,
        ).wait_recv()

    for d in (2, 3, 1, 0):
        to = (zl + d) % 4
        at = pl.ds(pl.multiple_of(to * TOK, 16), TOK)
        joined = None
        for s in range(4):
            piece = cin[s, at, :].astype(F32)
            wide = jnp.concatenate([piece, jnp.zeros((TOK, 384), F32)], axis=1)
            if s:
                wide = pltpu.roll(wide, 160 * s, 1)
            joined = wide if joined is None else joined + wide
        if d:
            zsend[d] = joined.astype(BF16)
            z_copy(d).start()
        else:
            ctx[half, :, pl.ds(pl.multiple_of(640 * part, 128), 640)] = joined.astype(BF16)

    ring_relay(3, 1)
    for i in (1, 2, 3):
        ring_end(i, 1)
    for d in (1, 2, 3):
        z_wait(d)

    rows = 2 * TOK
    sibling_wait(1, 0)
    sibling_wait(1, 1)

    @pl.loop(0, 5)
    def _(n):
        at = pl.ds(pl.multiple_of(256 * n, 256), 256)
        block = wout[:, :, :, :, at].reshape(D, 256)
        made = jnp.dot(ctx[...].reshape(rows, D), block, preferred_element_type=F32)
        mid[:, at] = x_ref[:, :, at].reshape(rows, 256).astype(F32) + made + out_bias[:, at]

    @pl.loop(0, rows // 16)
    def _(n):
        at = pl.ds(pl.multiple_of(n * 16, 16), 16)
        normed_mlp[at, :] = norm_rows(mid[at, :], mlp_gain, mlp_shift).astype(BF16)

    sibling_wait(2, 0)
    sibling_wait(2, 1)

    @pl.loop(0, 10)
    def _(n):
        at = pl.ds(pl.multiple_of(256 * n, 256), 256)
        block = wup[:, :, :, :, at].reshape(D, 256)
        lifted = jnp.dot(normed_mlp[...], block, preferred_element_type=F32) + up_bias[:, at]
        hid[:, at] = (0.5 * lifted * (1.0 + lax.erf(lifted * math.sqrt(0.5)))).astype(BF16)

    sibling_wait(3, 0)
    sibling_wait(3, 1)

    @pl.loop(0, 5)
    def _(n):
        at = pl.ds(pl.multiple_of(256 * n, 256), 256)
        block = wdown[:, :, :, :, at].reshape(FF, 256)
        lowered = jnp.dot(hid[...], block, preferred_element_type=F32)
        result = mid[:, at] + lowered + down_bias[:, at]
        o_ref[:, :, at] = result.astype(BF16).reshape(2, TOK, 256)

    for copy in started:
        copy.wait_send()
    to_partner.wait_send()
    to_near.wait_send()

    @pl.when(is_near)
    def _():
        to_far.wait_send()
        onward.wait_send()

    @pl.loop(0, 4)
    def _(slot):
        for r in (1, 2, 3):
            y_copy(r, slot).wait_send()

    for t, r in enumerate(order[:3]):
        c_copy(t, r).wait_send()
    for d in (1, 2, 3):
        z_copy(d).wait_send()


def layer(
    tokens, pre_gain, pre_shift, w_qkv, qkv_bias, w_out, out_bias,
    mlp_gain, mlp_shift, w_up, up_bias, w_down, down_bias,
):
    vmem = pl.BlockSpec(memory_space=pltpu.VMEM)
    hbm = pl.BlockSpec(memory_space=pltpu.HBM)
    dma = pltpu.SemaphoreType.DMA
    return pl.pallas_call(
        kernel,
        out_shape=jax.ShapeDtypeStruct((2, TOK, D), BF16),
        in_specs=[vmem] * 9 + [hbm] * 4,
        out_specs=vmem,
        scratch_shapes=[
            pltpu.VMEM((4, 2, 2, 80, HALF), BF16),
            pltpu.VMEM((4, 2, 2, 80, D), BF16),
            pltpu.VMEM((4, 2, 2, 80, FF), BF16),
            pltpu.VMEM((4, 2, 2, 160, D), BF16),
            pltpu.VMEM((4, TOK, D), BF16),
            pltpu.VMEM((TOK, D), BF16),
            pltpu.VMEM((TOK, HALF), F32),
            pltpu.VMEM((4, 4, TOK, 512), BF16),
            pltpu.VMEM((4, 4, TOK, 512), BF16),
            pltpu.VMEM((2, SEQ, 128), BF16),
            pltpu.VMEM((2, SEQ, 128), BF16),
            pltpu.VMEM((2, SEQ, 256), BF16),
            pltpu.VMEM((4, 4 * TOK, 256), BF16),
            pltpu.VMEM((4, 4 * TOK, 256), BF16),
            pltpu.VMEM((4, TOK, 640), BF16),
            pltpu.VMEM((2, TOK, D), BF16),
            pltpu.VMEM((2 * TOK, D), F32),
            pltpu.VMEM((2 * TOK, D), BF16),
            pltpu.VMEM((2 * TOK, FF), BF16),
            dma((4,)), dma((4, 12)), dma((4, 12)), dma((4,)), dma((4,)),
            dma((3, 4)), dma((3, 4)), dma((3,)), dma((3,)), dma((4,)), dma((4,)),
        ],
        compiler_params=pltpu.CompilerParams(
            collective_id=0, has_side_effects=True, vmem_limit_bytes=67043328
        ),
    )(
        tokens, pre_gain[None], pre_shift[None], qkv_bias.reshape(2, 1, HALF), out_bias[None],
        mlp_gain[None], mlp_shift[None], up_bias[None], down_bias[None],
        w_qkv, w_out, w_up, w_down,
    )


def solution(mesh):
    in_specs = (
        P("dp", "seq", None),
        P(), P(), P("dp", None), P(), P("dp", None), P(), P(), P(), P("dp", None), P(),
        P("dp", None), P(),
    )
    out_specs = P("dp", "seq", None)
    return jax.shard_map(layer, mesh=mesh, in_specs=in_specs, out_specs=out_specs, check_vma=False)
```

```python
import math

import jax
import jax.numpy as jnp
from jax import lax
from jax.experimental import pallas as pl
from jax.experimental.pallas import tpu as pltpu
from jax.sharding import PartitionSpec as P

D = 1280
HEADS = 16
HEAD_DIM = 80
FF = 2560
TOK = 144
SEQ = 2304
HALF = 1920
PAIR = 480
EPSILON = 1e-05
EXP_SCALE = math.log2(math.e) / math.sqrt(HEAD_DIM)

MESH = pl.DeviceIdType.MESH
F32 = jnp.float32
BF16 = jnp.bfloat16

COLS = (HALF, D, FF, D)
LOW = (1024, 640, 1280, 640)
ROWS = (80, 80, 80, 160)
XM, XP, X2L, X2R, ZC, YC, DC = 0, 1, 2, 3, 8, 9, 10


def kernel(
    x_ref, pre_gain, pre_shift, qkv_bias, out_bias, mlp_gain, mlp_shift, up_bias, down_bias,
    wqkv_in, wout_in, wup_in, wdown_in,
    o_ref,
    wqkv, wout, wup, wdown,
    tok, other, packed, qsend, qin, qb, kb, vb, score_a, score_b, csend, cin, zsend, ctx, mid, normed_mlp, hid,
    load_sem, w_send, w_recv, t_send, t_recv, y_send, y_recv, c_send, c_recv, z_send, z_recv,
):
    dp = lax.axis_index("dp")
    sq = lax.axis_index("seq")
    x, zh, c = dp // 4, (dp // 2) % 2, dp % 2
    zl, y = sq // 4, sq % 4
    half, part = zl // 2, zl % 2

    def dev(x=x, zh=zh, c=c, zl=zl, y=y):
        return ((x * 2 + zh) * 2 + c, zl * 4 + y)

    xr, xl, xo = (x + 1) % 4, (x + 3) % 4, (x + 2) % 4
    ypair = y + 1 - 2 * (y % 2)
    partner = zl + 1 - 2 * part
    near_here = 1 + half
    is_near = zl == near_here
    near_other = 2 - half
    far_other = 3 - 3 * half

    barrier = pltpu.get_barrier_semaphore()
    peers = [dev(x=xr), dev(x=xl), dev(zh=1 - zh), dev(c=1 - c)]
    peers += [dev(zl=(zl + d) % 4) for d in (1, 2, 3)]
    peers += [dev(y=(y + d) % 4) for d in (1, 2, 3)]

    bufs = (wqkv, wout, wup, wdown)
    sources = (
        wqkv_in.at[:, pl.ds(pl.multiple_of(part * HALF, 128), HALF)],
        wout_in,
        wup_in,
        wdown_in,
    )
    loads = [
        pltpu.make_async_copy(sources[i], bufs[i].at[x, zh, c], load_sem.at[i]) for i in range(4)
    ]
    for load in loads:
        load.start()
    for peer in peers:
        pl.semaphore_signal(barrier, inc=1, device_id=peer, device_id_type=MESH)
    pl.semaphore_wait(barrier, len(peers))

    started = []

    def region(i, xx, zz, cc, lo=0, size=None):
        size = COLS[i] if size is None else size
        return bufs[i].at[xx, zz, cc, :, pl.ds(lo, size)]

    def w_copy(i, j, ref, target):
        return pltpu.make_async_remote_copy(
            src_ref=ref, dst_ref=ref, send_sem=w_send.at[i, j], recv_sem=w_recv.at[i, j],
            device_id=target, device_id_type=MESH,
        )

    def w_start(i, j, ref, target):
        copy = w_copy(i, j, ref, target)
        copy.start()
        started.append(copy)

    def w_wait(i, j, ref):
        w_copy(i, j, ref, dev(c=1 - c)).wait_recv()

    def side(k):
        return zh if k == 0 else 1 - zh

    def ring_start(i, k):
        mine = region(i, x, side(k), c)
        w_start(i, 4 * k + XM, mine, dev(x=xr))
        w_start(i, 4 * k + XP, mine, dev(x=xl))

    def ring_relay(i, k):
        low, high = LOW[i], COLS[i] - LOW[i]
        w_wait(i, 4 * k + XM, region(i, xl, side(k), c))
        w_start(i, 4 * k + X2L, region(i, xl, side(k), c, 0, low), dev(x=xr))
        w_wait(i, 4 * k + XP, region(i, xr, side(k), c))
        w_start(i, 4 * k + X2R, region(i, xr, side(k), c, low, high), dev(x=xl))

    def ring_end(i, k):
        low, high = LOW[i], COLS[i] - LOW[i]
        w_wait(i, 4 * k + X2L, region(i, xo, side(k), c, 0, low))
        w_wait(i, 4 * k + X2R, region(i, xo, side(k), c, low, high))
        w_start(i, DC + k, bufs[i].at[:, side(k), c], dev(c=1 - c))

    def sibling_wait(i, k):
        w_wait(i, DC + k, bufs[i].at[:, side(k), 1 - c])

    def cut(i, which):
        size = LOW[i]
        return pl.multiple_of(which * size, 128), size

    def class_start(i):
        lo, size = cut(i, y % 2)
        w_start(i, ZC, region(i, x, zh, c, lo, size), dev(zh=1 - zh))

    def class_swap(i):
        lo, size = cut(i, y % 2)
        w_wait(i, ZC, region(i, x, 1 - zh, c, lo, size))
        w_start(i, YC, region(i, x, 1 - zh, c, lo, size), dev(y=ypair))

    def class_ring(i):
        lo, size = cut(i, 1 - y % 2)
        w_wait(i, YC, region(i, x, 1 - zh, c, lo, size))
        ring_start(i, 1)

    def uneven(which, j):
        lo, size = (0, LOW[0]) if which == 0 else (LOW[0], COLS[0] - LOW[0])
        if j == ZC:
            return w_copy(0, ZC, region(0, x, zh, c, lo, size), dev(zh=1 - zh))
        return w_copy(0, YC, region(0, x, 1 - zh, c, lo, size), dev(y=ypair))

    def by_parity(act):
        for which in (0, 1):

            @pl.when(y % 2 == which)
            def _():
                act(which)

    def first_start():
        by_parity(lambda which: uneven(which, ZC).start())

    def first_swap():
        def act(which):
            uneven(which, ZC).wait_recv()
            uneven(which, YC).start()

        by_parity(act)

    def first_ring():
        by_parity(lambda which: uneven(1 - which, YC).wait_recv())
        ring_start(0, 1)

    def first_sent():
        def act(which):
            uneven(which, ZC).wait_send()
            uneven(which, YC).wait_send()

        by_parity(act)

    loads[0].wait()
    first_start()
    ring_start(0, 0)

    def norm_rows(rows, gain, shift):
        average = jnp.mean(rows, axis=-1, keepdims=True)
        centered = rows - average
        spread = jnp.mean(centered * centered, axis=-1, keepdims=True)
        return centered * lax.rsqrt(spread + EPSILON) * gain[...] + shift[...]

    def norm_image(image, store):
        @pl.loop(0, TOK // 48)
        def _(n):
            at = pl.ds(pl.multiple_of(n * 48, 16), 48)
            rows = x_ref[image, at, :].astype(F32)
            store(at, norm_rows(rows, pre_gain, pre_shift).astype(BF16))

    def store_other(at, value):
        other[at, :] = value

    def store_own(at, value):
        tok[zl, at, :] = value

    def t_copy(src, slot, j, target):
        return pltpu.make_async_remote_copy(
            src_ref=src, dst_ref=tok.at[slot], send_sem=t_send.at[j], recv_sem=t_recv.at[slot],
            device_id=target, device_id_type=MESH,
        )

    norm_image(1 - half, store_other)
    to_near = t_copy(other, zl, 1, dev(zl=near_other))
    to_near.start()
    to_far = t_copy(other, zl, 2, dev(zl=far_other))

    @pl.when(is_near)
    def _():
        to_far.start()

    norm_image(half, store_own)
    to_partner = t_copy(tok.at[zl], zl, 0, dev(zl=partner))
    to_partner.start()

    for load in loads[1:]:
        load.wait()

    onward = t_copy(tok.at[far_other], far_other, 3, dev(zl=partner))

    def token_wait(slot):
        t_copy(tok.at[slot], slot, 0, dev(zl=partner)).wait_recv()

    first_swap()
    ring_relay(0, 0)
    first_ring()
    ring_end(0, 0)
    ring_relay(0, 1)
    for i in (1, 2, 3):
        ring_start(i, 0)

    @pl.when(is_near)
    def _():
        token_wait(far_other)
        onward.start()

    ring_end(0, 1)
    sibling_wait(0, 0)
    sibling_wait(0, 1)

    def slot_of(j):
        last = jnp.where(j == 2, near_other, far_other)
        return jnp.where(j == 0, zl, jnp.where(j == 1, partner, last))

    def y_copy(r, head, slot):
        to = (y + r) % 4
        return pltpu.make_async_remote_copy(
            src_ref=qsend.at[head, to, slot], dst_ref=qin.at[head, y, slot],
            send_sem=y_send.at[head, r - 1, slot], recv_sem=y_recv.at[head, r - 1, slot],
            device_id=dev(y=to), device_id_type=MESH,
        )

    def y_copy_in(r, head, slot, source):
        return pltpu.make_async_remote_copy(
            src_ref=qin.at[head, source, slot], dst_ref=qin.at[head, source, slot],
            send_sem=y_send.at[head, r - 1, slot], recv_sem=y_recv.at[head, r - 1, slot],
            device_id=dev(y=(y + 1) % 4), device_id_type=MESH,
        )

    @pl.loop(0, 4)
    def _(j):
        slot = slot_of(j)

        @pl.when((j > 0) & jnp.logical_not((j == 3) & is_near))
        def _():
            token_wait(slot)

        rows = tok[slot]
        bias_at = pl.multiple_of(part * HALF, 128)
        for n in range(3):
            at = slice(640 * n, 640 * n + 640)
            block = wqkv[:, :, :, :, at].reshape(D, 640)
            bias = qkv_bias[:, pl.ds(bias_at + 640 * n, 640)]
            packed[:, at] = jnp.dot(rows, block, preferred_element_type=F32) + bias
        for head in range(2):
            for to in range(4):
                first = PAIR * to + 240 * head
                start = first // 128 * 128
                wide = packed[:, start : min(start + 384, HALF)]
                shift = first - start
                if shift:
                    wide = pltpu.roll(wide, wide.shape[1] - shift, 1)
                qsend[head, to, slot] = wide[:, :256].astype(BF16)
            qin[head, y, slot] = qsend[head, y, slot]
        for r in (2, 1, 3):
            y_copy(r, 0, slot).start()

    @pl.loop(0, 4)
    def _(j):
        for r in (2, 1, 3):
            y_copy(r, 1, slot_of(j)).start()

    for i in (1, 2, 3):
        class_start(i)
    for i in (1, 2):
        ring_relay(i, 0)

    lane128 = lax.broadcasted_iota(jnp.int32, (TOK, 128), 1)

    def unpack(head):
        @pl.loop(0, 16)
        def _(n):
            j, r = n // 4, n % 4
            slot = slot_of(j)
            source = (y + 4 - r) % 4

            @pl.when(r > 0)
            def _():
                y_copy_in(r, head, slot, source).wait_recv()

            wide = qin[head, source, slot].astype(F32)
            at = pl.ds(pl.multiple_of((source * 4 + slot) * TOK, 16), TOK)
            keep = lane128 < HEAD_DIM
            keys = pltpu.roll(wide, 256 - 80, 1)[:, :128]
            values = pltpu.roll(wide, 256 - 160, 1)[:, :128]
            ones = jnp.where(lane128 == HEAD_DIM, 1.0, 0.0)
            qb[head, at, :] = jnp.where(keep, wide[:, :128], 0.0).astype(BF16)
            kb[head, at, :] = jnp.where(keep, keys, 0.0).astype(BF16)
            vb[head, at, :] = jnp.where(keep, values, ones).astype(BF16)

    order = (2, 1, 3, 0)

    def c_copy(head, t):
        to = (y + order[t]) % 4
        return pltpu.make_async_remote_copy(
            src_ref=csend.at[head, to], dst_ref=cin.at[head, y],
            send_sem=c_send.at[head, t], recv_sem=c_recv.at[head, t],
            device_id=dev(y=to), device_id_type=MESH,
        )

    def c_wait(head, t):
        source = (y + 4 - order[t]) % 4
        pltpu.make_async_remote_copy(
            src_ref=cin.at[head, source], dst_ref=cin.at[head, source],
            send_sem=c_send.at[head, t], recv_sem=c_recv.at[head, t],
            device_id=dev(y=(y + 1) % 4), device_id_type=MESH,
        ).wait_recv()

    wide_lane = lax.broadcasted_iota(jnp.int32, (4 * TOK, 128), 1)

    def score(head, t, scores):
        to = (y + order[t]) % 4
        at = pl.ds(pl.multiple_of(to * 4 * TOK, 16), 4 * TOK)
        scores[...] = lax.dot_general(
            qb[head, at, :], kb[head], (((1,), (1,)), ((), ())), preferred_element_type=F32
        )

    def mix(head, t, scores):
        to = (y + order[t]) % 4
        highest = jnp.max(scores[...], axis=-1, keepdims=True) * EXP_SCALE
        weights = jnp.exp2(scores[...] * EXP_SCALE - highest).astype(BF16)
        total = jnp.dot(weights, vb[head], preferred_element_type=F32)
        mixed = jnp.where(wide_lane < HEAD_DIM, total / total[:, HEAD_DIM : HEAD_DIM + 1], 0.0)
        csend[head, to] = mixed.astype(BF16)

    def attend(head):
        slots = (score_a, score_b)
        score(head, 0, slots[0])
        for t in range(4):
            if t < 3:
                score(head, t + 1, slots[(t + 1) % 2])
            mix(head, t, slots[t % 2])
            if t < 3:
                c_copy(head, t).start()
        cin[head, y] = csend[head, y]

    def z_place(of_half, of_part):
        return of_half, pl.ds(pl.multiple_of(384 * of_part, 128), 384)

    def z_copy(head, d):
        at_half, at = z_place(half, part)
        return pltpu.make_async_remote_copy(
            src_ref=zsend.at[head, d], dst_ref=ctx.at[head, at_half, :, at],
            send_sem=z_send.at[head, d], recv_sem=z_recv.at[head, d],
            device_id=dev(zl=(zl + d) % 4), device_id_type=MESH,
        )

    def z_wait(head):
        for d in (1, 2, 3):
            source = (zl + 4 - d) % 4
            at_half, at = z_place(source // 2, source % 2)
            ref = ctx.at[head, at_half, :, at]
            pltpu.make_async_remote_copy(
                src_ref=ref, dst_ref=ref, send_sem=z_send.at[head, d], recv_sem=z_recv.at[head, d],
                device_id=dev(zl=partner), device_id_type=MESH,
            ).wait_recv()

    def give_back(head):
        for t in range(3):
            c_wait(head, t)
        for d in (2, 3, 1, 0):
            to = (zl + d) % 4
            at = pl.ds(pl.multiple_of(to * TOK, 16), TOK)
            joined = None
            for s in range(4):
                piece = cin[head, s, at, :].astype(F32)
                wide = jnp.concatenate([piece, jnp.zeros((TOK, 256), F32)], axis=1)
                if s:
                    wide = pltpu.roll(wide, 80 * s, 1)
                joined = wide if joined is None else joined + wide
            if d:
                zsend[head, d] = joined.astype(BF16)
                z_copy(head, d).start()
            else:
                at_half, at = z_place(half, part)
                ctx[head, at_half, :, at] = joined.astype(BF16)

    rows = 2 * TOK

    def project(head):
        @pl.loop(0, 5)
        def _(n):
            at = pl.ds(pl.multiple_of(256 * n, 256), 256)
            made = None
            for p in range(2):
                block = wout[2 * p : 2 * p + 2, :, head, :, at].reshape(320, 256)
                left = ctx[head, :, :, 384 * p : 384 * p + 320].reshape(rows, 320)
                term = jnp.dot(left, block, preferred_element_type=F32)
                made = term if made is None else made + term
            if head == 0:
                mid[:, at] = x_ref[:, :, at].reshape(rows, 256).astype(F32) + made + out_bias[:, at]
            else:
                mid[:, at] += made

    unpack(0)
    ring_relay(3, 0)
    attend(0)
    for i in (1, 2, 3):
        ring_end(i, 0)
    class_swap(1)
    class_swap(2)
    give_back(0)
    unpack(1)
    class_ring(1)
    class_ring(2)
    class_swap(3)
    attend(1)
    class_ring(3)
    give_back(1)
    ring_relay(1, 1)
    ring_relay(2, 1)
    ring_relay(3, 1)
    ring_end(1, 1)
    sibling_wait(1, 0)
    sibling_wait(1, 1)
    z_wait(0)
    project(0)
    ring_end(2, 1)
    z_wait(1)
    project(1)

    @pl.loop(0, rows // 48)
    def _(n):
        at = pl.ds(pl.multiple_of(n * 48, 16), 48)
        normed_mlp[at, :] = norm_rows(mid[at, :], mlp_gain, mlp_shift).astype(BF16)

    ring_end(3, 1)
    sibling_wait(2, 0)
    sibling_wait(2, 1)

    @pl.loop(0, 10)
    def _(n):
        at = pl.ds(pl.multiple_of(256 * n, 256), 256)
        block = wup[:, :, :, :, at].reshape(D, 256)
        lifted = jnp.dot(normed_mlp[...], block, preferred_element_type=F32) + up_bias[:, at]
        hid[:, at] = (0.5 * lifted * (1.0 + lax.erf(lifted * math.sqrt(0.5)))).astype(BF16)

    sibling_wait(3, 0)
    sibling_wait(3, 1)

    @pl.loop(0, 5)
    def _(n):
        at = pl.ds(pl.multiple_of(256 * n, 256), 256)
        block = wdown[:, :, :, :, at].reshape(FF, 256)
        lowered = jnp.dot(hid[...], block, preferred_element_type=F32)
        result = mid[:, at] + lowered + down_bias[:, at]
        o_ref[:, :, at] = result.astype(BF16).reshape(2, TOK, 256)

    for copy in started:
        copy.wait_send()
    to_partner.wait_send()
    to_near.wait_send()

    @pl.when(is_near)
    def _():
        to_far.wait_send()
        onward.wait_send()

    @pl.loop(0, 4)
    def _(slot):
        for head in range(2):
            for r in (1, 2, 3):
                y_copy(r, head, slot).wait_send()

    for head in range(2):
        for t in range(3):
            c_copy(head, t).wait_send()
        for d in (1, 2, 3):
            z_copy(head, d).wait_send()
    first_sent()


def layer(
    tokens, pre_gain, pre_shift, w_qkv, qkv_bias, w_out, out_bias,
    mlp_gain, mlp_shift, w_up, up_bias, w_down, down_bias,
):
    vmem = pl.BlockSpec(memory_space=pltpu.VMEM)
    hbm = pl.BlockSpec(memory_space=pltpu.HBM)
    dma = pltpu.SemaphoreType.DMA
    vectors = (pre_gain, pre_shift, qkv_bias, out_bias, mlp_gain, mlp_shift, up_bias, down_bias)
    rows = [vector[None] for vector in vectors]
    return pl.pallas_call(
        kernel,
        out_shape=jax.ShapeDtypeStruct((2, TOK, D), BF16),
        in_specs=[vmem] * 9 + [hbm] * 4,
        out_specs=vmem,
        scratch_shapes=[
            pltpu.VMEM((4, 2, 2, 80, HALF), BF16),
            pltpu.VMEM((4, 2, 2, 80, D), BF16),
            pltpu.VMEM((4, 2, 2, 80, FF), BF16),
            pltpu.VMEM((4, 2, 2, 160, D), BF16),
            pltpu.VMEM((4, TOK, D), BF16),
            pltpu.VMEM((TOK, D), BF16),
            pltpu.VMEM((TOK, HALF), F32),
            pltpu.VMEM((2, 4, 4, TOK, 256), BF16),
            pltpu.VMEM((2, 4, 4, TOK, 256), BF16),
            pltpu.VMEM((2, SEQ, 128), BF16),
            pltpu.VMEM((2, SEQ, 128), BF16),
            pltpu.VMEM((2, SEQ, 128), BF16),
            pltpu.VMEM((4 * TOK, SEQ), F32),
            pltpu.VMEM((4 * TOK, SEQ), F32),
            pltpu.VMEM((2, 4, 4 * TOK, 128), BF16),
            pltpu.VMEM((2, 4, 4 * TOK, 128), BF16),
            pltpu.VMEM((2, 4, TOK, 384), BF16),
            pltpu.VMEM((2, 2, TOK, 768), BF16),
            pltpu.VMEM((2 * TOK, D), F32),
            pltpu.VMEM((2 * TOK, D), BF16),
            pltpu.VMEM((2 * TOK, FF), BF16),
            dma((4,)), dma((4, 12)), dma((4, 12)), dma((4,)), dma((4,)),
            dma((2, 3, 4)), dma((2, 3, 4)), dma((2, 3)), dma((2, 3)), dma((2, 4)), dma((2, 4)),
        ],
        compiler_params=pltpu.CompilerParams(
            collective_id=0, has_side_effects=True, vmem_limit_bytes=67043328
        ),
    )(
        tokens, *rows,
        w_qkv, w_out, w_up, w_down,
    )


def solution(mesh):
    in_specs = (
        P("dp", "seq", None),
        P(), P(), P("dp", None), P(), P("dp", None), P(), P(), P(), P("dp", None), P(),
        P("dp", None), P(),
    )
    out_specs = P("dp", "seq", None)
    return jax.shard_map(layer, mesh=mesh, in_specs=in_specs, out_specs=out_specs, check_vma=False)
```

```python
import math

import jax
import jax.numpy as jnp
from jax import lax
from jax.experimental import pallas as pl
from jax.experimental.pallas import tpu as pltpu
from jax.sharding import PartitionSpec as P

D = 1280
HEADS = 16
HEAD_DIM = 80
FF = 2560
TOK = 144
SEQ = 2304
HALF = 1920
PAIR = 480
EPSILON = 1e-05
EXP_SCALE = math.log2(math.e) / math.sqrt(HEAD_DIM)

MESH = pl.DeviceIdType.MESH
F32 = jnp.float32
BF16 = jnp.bfloat16

COLS = (HALF, D, FF, D)
LOW = (1024, 640, 1280, 640)
ROWS = (80, 80, 80, 160)
XM, XP, X2L, X2R, ZC, YC, YQ, DC = 0, 1, 2, 3, 8, 9, 10, 13


def kernel(
    x_ref, pre_gain, pre_shift, qkv_bias, out_bias, mlp_gain, mlp_shift, up_bias, down_bias,
    wqkv_in, wout_in, wup_in, wdown_in,
    o_ref,
    wqkv, wout, wup, wdown,
    tok, other, packed, qsend, qin, qb, kb, vb, score_a, score_b, csend, cin, zsend, ctx, mid, normed_mlp, hid,
    load_sem, w_send, w_recv, t_send, t_recv, y_send, y_recv, c_send, c_recv, z_send, z_recv,
):
    dp = lax.axis_index("dp")
    sq = lax.axis_index("seq")
    x, zh, c = dp // 4, (dp // 2) % 2, dp % 2
    zl, y = sq // 4, sq % 4
    half, part = zl // 2, zl % 2

    def dev(x=x, zh=zh, c=c, zl=zl, y=y):
        return ((x * 2 + zh) * 2 + c, zl * 4 + y)

    xr, xl, xo = (x + 1) % 4, (x + 3) % 4, (x + 2) % 4
    ypair = y + 1 - 2 * (y % 2)
    partner = zl + 1 - 2 * part
    near_here = 1 + half
    is_near = zl == near_here
    near_other = 2 - half
    far_other = 3 - 3 * half

    barrier = pltpu.get_barrier_semaphore()
    peers = [dev(x=xr), dev(x=xl), dev(zh=1 - zh), dev(c=1 - c)]
    peers += [dev(zl=(zl + d) % 4) for d in (1, 2, 3)]
    peers += [dev(y=(y + d) % 4) for d in (1, 2, 3)]

    bufs = (wqkv, wout, wup, wdown)
    sources = (
        wqkv_in.at[:, pl.ds(pl.multiple_of(part * HALF, 128), HALF)],
        wout_in,
        wup_in,
        wdown_in,
    )
    loads = [
        pltpu.make_async_copy(sources[i], bufs[i].at[x, zh, c], load_sem.at[i]) for i in range(4)
    ]
    for load in loads:
        load.start()
    for peer in peers:
        pl.semaphore_signal(barrier, inc=1, device_id=peer, device_id_type=MESH)
    pl.semaphore_wait(barrier, len(peers))

    started = []

    def region(i, xx, zz, cc, lo=0, size=None):
        size = COLS[i] if size is None else size
        return bufs[i].at[xx, zz, cc, :, pl.ds(lo, size)]

    def w_copy(i, j, ref, target):
        return pltpu.make_async_remote_copy(
            src_ref=ref, dst_ref=ref, send_sem=w_send.at[i, j], recv_sem=w_recv.at[i, j],
            device_id=target, device_id_type=MESH,
        )

    def w_start(i, j, ref, target):
        copy = w_copy(i, j, ref, target)
        copy.start()
        started.append(copy)

    def w_wait(i, j, ref):
        w_copy(i, j, ref, dev(c=1 - c)).wait_recv()

    def side(k):
        return zh if k == 0 else 1 - zh

    def to_sibling(i, k, n, xx):
        w_start(i, DC + 4 * k + n, region(i, xx, side(k), c), dev(c=1 - c))

    def ring_start(i, k):
        mine = region(i, x, side(k), c)
        w_start(i, 4 * k + XM, mine, dev(x=xr))
        w_start(i, 4 * k + XP, mine, dev(x=xl))
        to_sibling(i, k, 0, x)

    def ring_relay(i, k):
        low, high = LOW[i], COLS[i] - LOW[i]
        w_wait(i, 4 * k + XM, region(i, xl, side(k), c))
        w_start(i, 4 * k + X2L, region(i, xl, side(k), c, 0, low), dev(x=xr))
        to_sibling(i, k, 1, xl)
        w_wait(i, 4 * k + XP, region(i, xr, side(k), c))
        w_start(i, 4 * k + X2R, region(i, xr, side(k), c, low, high), dev(x=xl))
        to_sibling(i, k, 2, xr)

    def ring_end(i, k):
        low, high = LOW[i], COLS[i] - LOW[i]
        w_wait(i, 4 * k + X2L, region(i, xo, side(k), c, 0, low))
        w_wait(i, 4 * k + X2R, region(i, xo, side(k), c, low, high))
        to_sibling(i, k, 3, xo)

    def sibling_wait(i, k):
        for n, xx in enumerate((x, xl, xr, xo)):
            w_wait(i, DC + 4 * k + n, region(i, xx, side(k), 1 - c))

    def piece(i, zz, who):
        if i == 1:
            return region(i, x, zz, c, pl.multiple_of(640 * (who % 2), 128), 640)
        if i == 2:
            return region(i, x, zz, c, pl.multiple_of(640 * who, 128), 640)
        down = pl.ds(pl.multiple_of(80 * (who // 2), 16), 80)
        return bufs[i].at[x, zz, c, down, pl.ds(pl.multiple_of(640 * (who % 2), 128), 640)]

    def class_start(i):
        w_start(i, ZC, piece(i, zh, y), dev(zh=1 - zh))

    def class_swap(i):
        mine = piece(i, 1 - zh, y)
        w_wait(i, ZC, mine)
        if i == 1:
            w_start(i, YQ, mine, dev(y=ypair))
        else:
            for r in (2, 1, 3):
                w_start(i, YQ + r - 1, mine, dev(y=(y + r) % 4))

    def class_ring(i):
        if i == 1:
            w_wait(i, YQ, piece(i, 1 - zh, ypair))
        else:
            for r in (1, 2, 3):
                w_wait(i, YQ + r - 1, piece(i, 1 - zh, (y + 4 - r) % 4))
        ring_start(i, 1)

    def uneven(which, j):
        lo, size = (0, LOW[0]) if which == 0 else (LOW[0], COLS[0] - LOW[0])
        if j == ZC:
            return w_copy(0, ZC, region(0, x, zh, c, lo, size), dev(zh=1 - zh))
        return w_copy(0, YC, region(0, x, 1 - zh, c, lo, size), dev(y=ypair))

    def by_parity(act):
        for which in (0, 1):

            @pl.when(y % 2 == which)
            def _():
                act(which)

    def first_start():
        by_parity(lambda which: uneven(which, ZC).start())

    def first_swap():
        def act(which):
            uneven(which, ZC).wait_recv()
            uneven(which, YC).start()

        by_parity(act)

    def first_ring():
        by_parity(lambda which: uneven(1 - which, YC).wait_recv())
        ring_start(0, 1)

    def first_sent():
        def act(which):
            uneven(which, ZC).wait_send()
            uneven(which, YC).wait_send()

        by_parity(act)

    loads[0].wait()
    first_start()
    ring_start(0, 0)

    def row_of(ref, at=slice(None)):
        return ref[at].reshape(1, -1)

    def norm_rows(rows, gain, shift):
        average = jnp.mean(rows, axis=-1, keepdims=True)
        centered = rows - average
        spread = jnp.mean(centered * centered, axis=-1, keepdims=True)
        return centered * lax.rsqrt(spread + EPSILON) * row_of(gain) + row_of(shift)

    def norm_image(image, store):
        @pl.loop(0, TOK // 48)
        def _(n):
            at = pl.ds(pl.multiple_of(n * 48, 16), 48)
            rows = x_ref[image, at, :].astype(F32)
            store(at, norm_rows(rows, pre_gain, pre_shift).astype(BF16))

    def store_other(at, value):
        other[at, :] = value

    def store_own(at, value):
        tok[zl, at, :] = value

    def t_copy(src, slot, j, target):
        return pltpu.make_async_remote_copy(
            src_ref=src, dst_ref=tok.at[slot], send_sem=t_send.at[j], recv_sem=t_recv.at[slot],
            device_id=target, device_id_type=MESH,
        )

    norm_image(1 - half, store_other)
    to_near = t_copy(other, zl, 1, dev(zl=near_other))
    to_near.start()
    to_far = t_copy(other, zl, 2, dev(zl=far_other))

    @pl.when(is_near)
    def _():
        to_far.start()

    norm_image(half, store_own)
    to_partner = t_copy(tok.at[zl], zl, 0, dev(zl=partner))
    to_partner.start()

    for load in loads[1:]:
        load.wait()
    class_start(1)

    onward = t_copy(tok.at[far_other], far_other, 3, dev(zl=partner))

    def token_wait(slot):
        t_copy(tok.at[slot], slot, 0, dev(zl=partner)).wait_recv()

    first_swap()
    ring_relay(0, 0)
    first_ring()
    ring_end(0, 0)
    ring_relay(0, 1)
    for i in (1, 2, 3):
        ring_start(i, 0)

    @pl.when(is_near)
    def _():
        token_wait(far_other)
        onward.start()

    ring_end(0, 1)
    class_swap(1)
    sibling_wait(0, 0)
    sibling_wait(0, 1)

    def slot_of(j):
        last = jnp.where(j == 2, near_other, far_other)
        return jnp.where(j == 0, zl, jnp.where(j == 1, partner, last))

    def y_copy(r, head, slot):
        to = (y + r) % 4
        return pltpu.make_async_remote_copy(
            src_ref=qsend.at[head, to, slot], dst_ref=qin.at[head, y, slot],
            send_sem=y_send.at[head, r - 1, slot], recv_sem=y_recv.at[head, r - 1, slot],
            device_id=dev(y=to), device_id_type=MESH,
        )

    def y_copy_in(r, head, slot, source):
        return pltpu.make_async_remote_copy(
            src_ref=qin.at[head, source, slot], dst_ref=qin.at[head, source, slot],
            send_sem=y_send.at[head, r - 1, slot], recv_sem=y_recv.at[head, r - 1, slot],
            device_id=dev(y=(y + 1) % 4), device_id_type=MESH,
        )

    def first_projection(j):
        slot = slot_of(j)

        @pl.when((j > 0) & jnp.logical_not((j == 3) & is_near))
        def _():
            token_wait(slot)

        rows = tok[slot]
        bias_at = pl.multiple_of(part * HALF, 128)
        for n in range(3):
            at = slice(640 * n, 640 * n + 640)
            block = wqkv[:, :, :, :, at].reshape(D, 640)
            bias = row_of(qkv_bias, pl.ds(bias_at + 640 * n, 640))
            packed[:, at] = jnp.dot(rows, block, preferred_element_type=F32) + bias
        for head in range(2):
            for to in range(4):
                first = PAIR * to + 240 * head
                start = first // 128 * 128
                wide = packed[:, start : min(start + 384, HALF)]
                shift = first - start
                if shift:
                    wide = pltpu.roll(wide, wide.shape[1] - shift, 1)
                qsend[head, to, slot] = wide[:, :256].astype(BF16)
            qin[head, y, slot] = qsend[head, y, slot]
        for r in (2, 1, 3):
            y_copy(r, 0, slot).start()

    pl.loop(0, 4)(first_projection)

    @pl.loop(0, 4)
    def _(j):
        for r in (2, 1, 3):
            y_copy(r, 1, slot_of(j)).start()

    class_start(2)
    class_start(3)
    for i in (1, 2):
        ring_relay(i, 0)
    class_ring(1)

    lane128 = lax.broadcasted_iota(jnp.int32, (TOK, 128), 1)

    def unpack(head):
        @pl.loop(0, 16)
        def _(n):
            j, r = n // 4, n % 4
            slot = slot_of(j)
            source = (y + 4 - r) % 4

            @pl.when(r > 0)
            def _():
                y_copy_in(r, head, slot, source).wait_recv()

            wide = qin[head, source, slot].astype(F32)
            at = pl.ds(pl.multiple_of((source * 4 + slot) * TOK, 16), TOK)
            keep = lane128 < HEAD_DIM
            keys = pltpu.roll(wide, 256 - 80, 1)[:, :128]
            values = pltpu.roll(wide, 256 - 160, 1)[:, :128]
            ones = jnp.where(lane128 == HEAD_DIM, 1.0, 0.0)
            qb[head, at, :] = jnp.where(keep, wide[:, :128], 0.0).astype(BF16)
            kb[head, at, :] = jnp.where(keep, keys, 0.0).astype(BF16)
            vb[head, at, :] = jnp.where(keep, values, ones).astype(BF16)

    order = (2, 1, 3, 0)

    def c_copy(head, t):
        to = (y + order[t]) % 4
        return pltpu.make_async_remote_copy(
            src_ref=csend.at[head, to], dst_ref=cin.at[head, y],
            send_sem=c_send.at[head, t], recv_sem=c_recv.at[head, t],
            device_id=dev(y=to), device_id_type=MESH,
        )

    def c_wait(head, t):
        source = (y + 4 - order[t]) % 4
        pltpu.make_async_remote_copy(
            src_ref=cin.at[head, source], dst_ref=cin.at[head, source],
            send_sem=c_send.at[head, t], recv_sem=c_recv.at[head, t],
            device_id=dev(y=(y + 1) % 4), device_id_type=MESH,
        ).wait_recv()

    wide_lane = lax.broadcasted_iota(jnp.int32, (4 * TOK, 128), 1)

    def score(head, t, scores):
        to = (y + order[t]) % 4
        at = pl.ds(pl.multiple_of(to * 4 * TOK, 16), 4 * TOK)
        scores[...] = lax.dot_general(
            qb[head, at, :], kb[head], (((1,), (1,)), ((), ())), preferred_element_type=F32
        )

    def mix(head, t, scores):
        to = (y + order[t]) % 4
        highest = jnp.max(scores[...], axis=-1, keepdims=True) * EXP_SCALE
        weights = jnp.exp2(scores[...] * EXP_SCALE - highest).astype(BF16)
        total = jnp.dot(weights, vb[head], preferred_element_type=F32)
        mixed = jnp.where(wide_lane < HEAD_DIM, total / total[:, HEAD_DIM : HEAD_DIM + 1], 0.0)
        csend[head, to] = mixed.astype(BF16)

    def attend(head, between):
        slots = (score_a, score_b)
        score(head, 0, slots[0])
        for t in range(4):
            if t < 3:
                score(head, t + 1, slots[(t + 1) % 2])
            mix(head, t, slots[t % 2])
            if t < 3:
                c_copy(head, t).start()
            if t in between:
                between[t]()
        cin[head, y] = csend[head, y]

    def z_place(of_half, of_part):
        return of_half, pl.ds(pl.multiple_of(384 * of_part, 128), 384)

    def z_copy(head, d):
        at_half, at = z_place(half, part)
        return pltpu.make_async_remote_copy(
            src_ref=zsend.at[head, d], dst_ref=ctx.at[head, at_half, :, at],
            send_sem=z_send.at[head, d], recv_sem=z_recv.at[head, d],
            device_id=dev(zl=(zl + d) % 4), device_id_type=MESH,
        )

    def z_wait(head):
        for d in (1, 2, 3):
            source = (zl + 4 - d) % 4
            at_half, at = z_place(source // 2, source % 2)
            ref = ctx.at[head, at_half, :, at]
            pltpu.make_async_remote_copy(
                src_ref=ref, dst_ref=ref, send_sem=z_send.at[head, d], recv_sem=z_recv.at[head, d],
                device_id=dev(zl=partner), device_id_type=MESH,
            ).wait_recv()

    def give_back(head):
        for t in range(3):
            c_wait(head, t)
        for d in (2, 3, 1, 0):
            to = (zl + d) % 4
            at = pl.ds(pl.multiple_of(to * TOK, 16), TOK)
            joined = None
            for s in range(4):
                piece = cin[head, s, at, :].astype(F32)
                wide = jnp.concatenate([piece, jnp.zeros((TOK, 256), F32)], axis=1)
                if s:
                    wide = pltpu.roll(wide, 80 * s, 1)
                joined = wide if joined is None else joined + wide
            if d:
                zsend[head, d] = joined.astype(BF16)
                z_copy(head, d).start()
            else:
                at_half, at = z_place(half, part)
                ctx[head, at_half, :, at] = joined.astype(BF16)

    rows = 2 * TOK

    def project(head):
        @pl.loop(0, 5)
        def _(n):
            at = pl.ds(pl.multiple_of(256 * n, 256), 256)
            made = None
            for p in range(2):
                block = wout[2 * p : 2 * p + 2, :, head, :, at].reshape(320, 256)
                left = ctx[head, :, :, 384 * p : 384 * p + 320].reshape(rows, 320)
                term = jnp.dot(left, block, preferred_element_type=F32)
                made = term if made is None else made + term
            if head == 0:
                mid[:, at] = x_ref[:, :, at].reshape(rows, 256).astype(F32) + made + row_of(out_bias, at)
            else:
                mid[:, at] += made

    unpack(0)
    class_swap(2)
    ring_relay(3, 0)
    attend(0, {1: lambda: ring_end(1, 0), 2: lambda: ring_end(2, 0)})
    ring_relay(1, 1)
    class_swap(3)
    unpack(1)
    attend(1, {1: lambda: class_ring(2)})
    give_back(0)
    class_ring(3)
    give_back(1)
    ring_relay(2, 1)
    ring_end(3, 0)
    ring_end(1, 1)
    sibling_wait(1, 0)
    sibling_wait(1, 1)
    z_wait(0)
    project(0)
    z_wait(1)
    project(1)
    ring_relay(3, 1)
    ring_end(2, 1)

    @pl.loop(0, rows // 48)
    def _(n):
        at = pl.ds(pl.multiple_of(n * 48, 16), 48)
        normed_mlp[at, :] = norm_rows(mid[at, :], mlp_gain, mlp_shift).astype(BF16)

    sibling_wait(2, 0)
    sibling_wait(2, 1)

    @pl.loop(0, 10)
    def _(n):
        at = pl.ds(pl.multiple_of(256 * n, 256), 256)
        block = wup[:, :, :, :, at].reshape(D, 256)
        lifted = jnp.dot(normed_mlp[...], block, preferred_element_type=F32) + row_of(up_bias, at)
        hid[:, at] = (0.5 * lifted * (1.0 + lax.erf(lifted * math.sqrt(0.5)))).astype(BF16)

    ring_end(3, 1)
    sibling_wait(3, 0)
    sibling_wait(3, 1)

    @pl.loop(0, 5)
    def _(n):
        at = pl.ds(pl.multiple_of(256 * n, 256), 256)
        block = wdown[:, :, :, :, at].reshape(FF, 256)
        lowered = jnp.dot(hid[...], block, preferred_element_type=F32)
        result = mid[:, at] + lowered + row_of(down_bias, at)
        o_ref[:, :, at] = result.astype(BF16).reshape(2, TOK, 256)

    for copy in started:
        copy.wait_send()
    to_partner.wait_send()
    to_near.wait_send()

    @pl.when(is_near)
    def _():
        to_far.wait_send()
        onward.wait_send()

    @pl.loop(0, 4)
    def _(slot):
        for head in range(2):
            for r in (1, 2, 3):
                y_copy(r, head, slot).wait_send()

    for head in range(2):
        for t in range(3):
            c_copy(head, t).wait_send()
        for d in (1, 2, 3):
            z_copy(head, d).wait_send()
    first_sent()


def layer(
    tokens, pre_gain, pre_shift, w_qkv, qkv_bias, w_out, out_bias,
    mlp_gain, mlp_shift, w_up, up_bias, w_down, down_bias,
):
    vmem = pl.BlockSpec(memory_space=pltpu.VMEM)
    hbm = pl.BlockSpec(memory_space=pltpu.HBM)
    dma = pltpu.SemaphoreType.DMA
    vectors = (pre_gain, pre_shift, qkv_bias, out_bias, mlp_gain, mlp_shift, up_bias, down_bias)
    return pl.pallas_call(
        kernel,
        out_shape=jax.ShapeDtypeStruct((2, TOK, D), BF16),
        in_specs=[vmem] * 9 + [hbm] * 4,
        out_specs=vmem,
        scratch_shapes=[
            pltpu.VMEM((4, 2, 2, 80, HALF), BF16),
            pltpu.VMEM((4, 2, 2, 80, D), BF16),
            pltpu.VMEM((4, 2, 2, 80, FF), BF16),
            pltpu.VMEM((4, 2, 2, 160, D), BF16),
            pltpu.VMEM((4, TOK, D), BF16),
            pltpu.VMEM((TOK, D), BF16),
            pltpu.VMEM((TOK, HALF), F32),
            pltpu.VMEM((2, 4, 4, TOK, 256), BF16),
            pltpu.VMEM((2, 4, 4, TOK, 256), BF16),
            pltpu.VMEM((2, SEQ, 128), BF16),
            pltpu.VMEM((2, SEQ, 128), BF16),
            pltpu.VMEM((2, SEQ, 128), BF16),
            pltpu.VMEM((4 * TOK, SEQ), F32),
            pltpu.VMEM((4 * TOK, SEQ), F32),
            pltpu.VMEM((2, 4, 4 * TOK, 128), BF16),
            pltpu.VMEM((2, 4, 4 * TOK, 128), BF16),
            pltpu.VMEM((2, 4, TOK, 384), BF16),
            pltpu.VMEM((2, 2, TOK, 768), BF16),
            pltpu.VMEM((2 * TOK, D), F32),
            pltpu.VMEM((2 * TOK, D), BF16),
            pltpu.VMEM((2 * TOK, FF), BF16),
            dma((4,)), dma((4, 21)), dma((4, 21)), dma((4,)), dma((4,)),
            dma((2, 3, 4)), dma((2, 3, 4)), dma((2, 3)), dma((2, 3)), dma((2, 4)), dma((2, 4)),
        ],
        compiler_params=pltpu.CompilerParams(
            collective_id=0, has_side_effects=True, vmem_limit_bytes=67043328
        ),
    )(
        tokens, *vectors,
        w_qkv, w_out, w_up, w_down,
    )


def solution(mesh):
    in_specs = (
        P("dp", "seq", None),
        P(), P(), P("dp", None), P(), P("dp", None), P(), P(), P(), P("dp", None), P(),
        P("dp", None), P(),
    )
    out_specs = P("dp", "seq", None)
    return jax.shard_map(layer, mesh=mesh, in_specs=in_specs, out_specs=out_specs, check_vma=False)
```

```python
import math

import jax
import jax.numpy as jnp
from jax import lax
from jax.experimental import pallas as pl
from jax.experimental.pallas import tpu as pltpu
from jax.sharding import PartitionSpec as P

D = 1280
HEADS = 16
HEAD_DIM = 80
FF = 2560
TOK = 144
SEQ = 2304
HALF = 1920
PAIR = 480
EPSILON = 1e-05
EXP_SCALE = math.log2(math.e) / math.sqrt(HEAD_DIM)

MESH = pl.DeviceIdType.MESH
F32 = jnp.float32
BF16 = jnp.bfloat16

COLS = (HALF, D, FF, D)
LOW = (1024, 640, 1280, 640)
ROWS = (80, 80, 80, 160)
XM, XP, X2L, X2R, ZC, YC, YQ, DC = 0, 1, 2, 3, 8, 9, 10, 13


def kernel(
    x_in, pre_gain_in, pre_shift_in, qkv_bias_in, out_bias_in, mlp_gain_in, mlp_shift_in,
    up_bias_in, down_bias_in,
    wqkv_in, wout_in, wup_in, wdown_in,
    o_ref,
    x_ref, pre_gain, pre_shift, qkv_bias, out_bias, mlp_gain, mlp_shift, up_bias, down_bias,
    wqkv, wout, wup, wdown,
    tok, other, packed, qsend, qin, qb, kb, vb, score_a, score_b, csend, cin, zsend, ctx, mid, normed_mlp, hid,
    load_sem, w_send, w_recv, t_send, t_recv, y_send, y_recv, c_send, c_recv, z_send, z_recv,
):
    dp = lax.axis_index("dp")
    sq = lax.axis_index("seq")
    x, zh, c = dp // 4, (dp // 2) % 2, dp % 2
    zl, y = sq // 4, sq % 4
    half, part = zl // 2, zl % 2

    def dev(x=x, zh=zh, c=c, zl=zl, y=y):
        return ((x * 2 + zh) * 2 + c, zl * 4 + y)

    xr, xl, xo = (x + 1) % 4, (x + 3) % 4, (x + 2) % 4
    ypair = y + 1 - 2 * (y % 2)
    partner = zl + 1 - 2 * part
    near_here = 1 + half
    is_near = zl == near_here
    near_other = 2 - half
    far_other = 3 - 3 * half

    barrier = pltpu.get_barrier_semaphore()
    peers = [dev(x=xr), dev(x=xl), dev(zh=1 - zh), dev(c=1 - c)]
    peers += [dev(zl=(zl + d) % 4) for d in (1, 2, 3)]
    peers += [dev(y=(y + d) % 4) for d in (1, 2, 3)]

    bufs = (wqkv, wout, wup, wdown)
    sources = (
        wqkv_in.at[:, pl.ds(pl.multiple_of(part * HALF, 128), HALF)],
        wout_in,
        wup_in,
        wdown_in,
    )
    loads = [
        pltpu.make_async_copy(sources[i], bufs[i].at[x, zh, c], load_sem.at[i]) for i in range(4)
    ]
    early_in = (x_in, pre_gain_in, pre_shift_in)
    late_in = (qkv_bias_in, out_bias_in, mlp_gain_in, mlp_shift_in, up_bias_in, down_bias_in)
    early_to = (x_ref, pre_gain, pre_shift)
    late_to = (qkv_bias, out_bias, mlp_gain, mlp_shift, up_bias, down_bias)
    early = [
        pltpu.make_async_copy(a, b, load_sem.at[4 + n])
        for n, (a, b) in enumerate(zip(early_in, early_to))
    ]
    late = [
        pltpu.make_async_copy(a, b, load_sem.at[7 + n])
        for n, (a, b) in enumerate(zip(late_in, late_to))
    ]
    for peer in peers:
        pl.semaphore_signal(barrier, inc=1, device_id=peer, device_id_type=MESH)
    for load in (loads[0], *early, *loads[1:], *late):
        load.start()

    started = []

    def region(i, xx, zz, cc, lo=0, size=None):
        size = COLS[i] if size is None else size
        return bufs[i].at[xx, zz, cc, :, pl.ds(lo, size)]

    def w_copy(i, j, ref, target):
        return pltpu.make_async_remote_copy(
            src_ref=ref, dst_ref=ref, send_sem=w_send.at[i, j], recv_sem=w_recv.at[i, j],
            device_id=target, device_id_type=MESH,
        )

    def w_start(i, j, ref, target):
        copy = w_copy(i, j, ref, target)
        copy.start()
        started.append(copy)

    def w_wait(i, j, ref):
        w_copy(i, j, ref, dev(c=1 - c)).wait_recv()

    def side(k):
        return zh if k == 0 else 1 - zh

    def to_sibling(i, k, n, xx):
        w_start(i, DC + 4 * k + n, region(i, xx, side(k), c), dev(c=1 - c))

    def ring_start(i, k):
        mine = region(i, x, side(k), c)
        w_start(i, 4 * k + XM, mine, dev(x=xr))
        w_start(i, 4 * k + XP, mine, dev(x=xl))
        to_sibling(i, k, 0, x)

    def ring_relay(i, k):
        low, high = LOW[i], COLS[i] - LOW[i]
        w_wait(i, 4 * k + XM, region(i, xl, side(k), c))
        w_start(i, 4 * k + X2L, region(i, xl, side(k), c, 0, low), dev(x=xr))
        to_sibling(i, k, 1, xl)
        w_wait(i, 4 * k + XP, region(i, xr, side(k), c))
        w_start(i, 4 * k + X2R, region(i, xr, side(k), c, low, high), dev(x=xl))
        to_sibling(i, k, 2, xr)

    def ring_end(i, k):
        low, high = LOW[i], COLS[i] - LOW[i]
        w_wait(i, 4 * k + X2L, region(i, xo, side(k), c, 0, low))
        w_wait(i, 4 * k + X2R, region(i, xo, side(k), c, low, high))
        to_sibling(i, k, 3, xo)

    def sibling_wait(i, k):
        for n, xx in enumerate((x, xl, xr, xo)):
            w_wait(i, DC + 4 * k + n, region(i, xx, side(k), 1 - c))

    def piece(i, zz, who):
        if i == 1:
            return region(i, x, zz, c, pl.multiple_of(640 * (who % 2), 128), 640)
        if i == 2:
            return region(i, x, zz, c, pl.multiple_of(640 * who, 128), 640)
        down = pl.ds(pl.multiple_of(80 * (who // 2), 16), 80)
        return bufs[i].at[x, zz, c, down, pl.ds(pl.multiple_of(640 * (who % 2), 128), 640)]

    def class_start(i):
        w_start(i, ZC, piece(i, zh, y), dev(zh=1 - zh))

    def class_swap(i):
        mine = piece(i, 1 - zh, y)
        w_wait(i, ZC, mine)
        if i == 1:
            w_start(i, YQ, mine, dev(y=ypair))
        else:
            for r in (2, 1, 3):
                w_start(i, YQ + r - 1, mine, dev(y=(y + r) % 4))

    def class_ring(i):
        if i == 1:
            w_wait(i, YQ, piece(i, 1 - zh, ypair))
        else:
            for r in (1, 2, 3):
                w_wait(i, YQ + r - 1, piece(i, 1 - zh, (y + 4 - r) % 4))
        ring_start(i, 1)

    def uneven(which, j):
        lo, size = (0, LOW[0]) if which == 0 else (LOW[0], COLS[0] - LOW[0])
        if j == ZC:
            return w_copy(0, ZC, region(0, x, zh, c, lo, size), dev(zh=1 - zh))
        return w_copy(0, YC, region(0, x, 1 - zh, c, lo, size), dev(y=ypair))

    def by_parity(act):
        for which in (0, 1):

            @pl.when(y % 2 == which)
            def _():
                act(which)

    def first_start():
        by_parity(lambda which: uneven(which, ZC).start())

    def first_swap():
        def act(which):
            uneven(which, ZC).wait_recv()
            uneven(which, YC).start()

        by_parity(act)

    def first_ring():
        by_parity(lambda which: uneven(1 - which, YC).wait_recv())
        ring_start(0, 1)

    def first_sent():
        def act(which):
            uneven(which, ZC).wait_send()
            uneven(which, YC).wait_send()

        by_parity(act)

    def row_of(ref, at=slice(None)):
        return ref[at].reshape(1, -1)

    def norm_rows(rows, gain, shift):
        average = jnp.mean(rows, axis=-1, keepdims=True)
        centered = rows - average
        spread = jnp.mean(centered * centered, axis=-1, keepdims=True)
        return centered * lax.rsqrt(spread + EPSILON) * row_of(gain) + row_of(shift)

    def norm_image(image, store):
        @pl.loop(0, TOK // 48)
        def _(n):
            at = pl.ds(pl.multiple_of(n * 48, 16), 48)
            rows = x_ref[image, at, :].astype(F32)
            store(at, norm_rows(rows, pre_gain, pre_shift).astype(BF16))

    def store_other(at, value):
        other[at, :] = value

    def store_own(at, value):
        tok[zl, at, :] = value

    def t_copy(src, slot, j, target):
        return pltpu.make_async_remote_copy(
            src_ref=src, dst_ref=tok.at[slot], send_sem=t_send.at[j], recv_sem=t_recv.at[slot],
            device_id=target, device_id_type=MESH,
        )

    for load in early:
        load.wait()
    norm_image(1 - half, store_other)
    norm_image(half, store_own)
    loads[0].wait()
    pl.semaphore_wait(barrier, len(peers))

    first_start()
    ring_start(0, 0)
    to_near = t_copy(other, zl, 1, dev(zl=near_other))
    to_near.start()
    to_far = t_copy(other, zl, 2, dev(zl=far_other))

    @pl.when(is_near)
    def _():
        to_far.start()

    to_partner = t_copy(tok.at[zl], zl, 0, dev(zl=partner))
    to_partner.start()

    for load in (*loads[1:], *late):
        load.wait()
    class_start(1)

    onward = t_copy(tok.at[far_other], far_other, 3, dev(zl=partner))

    def token_wait(slot):
        t_copy(tok.at[slot], slot, 0, dev(zl=partner)).wait_recv()

    first_swap()
    ring_relay(0, 0)
    first_ring()
    ring_end(0, 0)
    ring_relay(0, 1)
    for i in (1, 2, 3):
        ring_start(i, 0)

    @pl.when(is_near)
    def _():
        token_wait(far_other)
        onward.start()

    ring_end(0, 1)
    class_swap(1)
    sibling_wait(0, 0)
    sibling_wait(0, 1)

    def slot_of(j):
        last = jnp.where(j == 2, near_other, far_other)
        return jnp.where(j == 0, zl, jnp.where(j == 1, partner, last))

    def y_copy(r, head, slot):
        to = (y + r) % 4
        return pltpu.make_async_remote_copy(
            src_ref=qsend.at[head, to, slot], dst_ref=qin.at[head, y, slot],
            send_sem=y_send.at[head, r - 1, slot], recv_sem=y_recv.at[head, r - 1, slot],
            device_id=dev(y=to), device_id_type=MESH,
        )

    def y_copy_in(r, head, slot, source):
        return pltpu.make_async_remote_copy(
            src_ref=qin.at[head, source, slot], dst_ref=qin.at[head, source, slot],
            send_sem=y_send.at[head, r - 1, slot], recv_sem=y_recv.at[head, r - 1, slot],
            device_id=dev(y=(y + 1) % 4), device_id_type=MESH,
        )

    def first_projection(j):
        slot = slot_of(j)

        @pl.when((j > 0) & jnp.logical_not((j == 3) & is_near))
        def _():
            token_wait(slot)

        rows = tok[slot]
        bias_at = pl.multiple_of(part * HALF, 128)
        for n in range(3):
            at = slice(640 * n, 640 * n + 640)
            block = wqkv[:, :, :, :, at].reshape(D, 640)
            bias = row_of(qkv_bias, pl.ds(bias_at + 640 * n, 640))
            packed[:, at] = jnp.dot(rows, block, preferred_element_type=F32) + bias
        for head in range(2):
            for to in range(4):
                first = PAIR * to + 240 * head
                start = first // 128 * 128
                wide = packed[:, start : min(start + 384, HALF)]
                shift = first - start
                if shift:
                    wide = pltpu.roll(wide, wide.shape[1] - shift, 1)
                qsend[head, to, slot] = wide[:, :256].astype(BF16)
            qin[head, y, slot] = qsend[head, y, slot]
        for r in (2, 1, 3):
            y_copy(r, 0, slot).start()

    pl.loop(0, 4)(first_projection)

    @pl.loop(0, 4)
    def _(j):
        for r in (2, 1, 3):
            y_copy(r, 1, slot_of(j)).start()

    class_start(2)
    class_start(3)
    for i in (1, 2):
        ring_relay(i, 0)
    class_ring(1)

    lane128 = lax.broadcasted_iota(jnp.int32, (TOK, 128), 1)

    def unpack(head):
        @pl.loop(0, 16)
        def _(n):
            j, r = n // 4, n % 4
            slot = slot_of(j)
            source = (y + 4 - r) % 4

            @pl.when(r > 0)
            def _():
                y_copy_in(r, head, slot, source).wait_recv()

            wide = qin[head, source, slot].astype(F32)
            at = pl.ds(pl.multiple_of((source * 4 + slot) * TOK, 16), TOK)
            keep = lane128 < HEAD_DIM
            keys = pltpu.roll(wide, 256 - 80, 1)[:, :128]
            values = pltpu.roll(wide, 256 - 160, 1)[:, :128]
            ones = jnp.where(lane128 == HEAD_DIM, 1.0, 0.0)
            qb[head, at, :] = jnp.where(keep, wide[:, :128], 0.0).astype(BF16)
            kb[head, at, :] = jnp.where(keep, keys, 0.0).astype(BF16)
            vb[head, at, :] = jnp.where(keep, values, ones).astype(BF16)

    order = (2, 1, 3, 0)

    def c_copy(head, t):
        to = (y + order[t]) % 4
        return pltpu.make_async_remote_copy(
            src_ref=csend.at[head, to], dst_ref=cin.at[head, y],
            send_sem=c_send.at[head, t], recv_sem=c_recv.at[head, t],
            device_id=dev(y=to), device_id_type=MESH,
        )

    def c_wait(head, t):
        source = (y + 4 - order[t]) % 4
        pltpu.make_async_remote_copy(
            src_ref=cin.at[head, source], dst_ref=cin.at[head, source],
            send_sem=c_send.at[head, t], recv_sem=c_recv.at[head, t],
            device_id=dev(y=(y + 1) % 4), device_id_type=MESH,
        ).wait_recv()

    wide_lane = lax.broadcasted_iota(jnp.int32, (4 * TOK, 128), 1)

    def score(head, t, scores):
        to = (y + order[t]) % 4
        at = pl.ds(pl.multiple_of(to * 4 * TOK, 16), 4 * TOK)
        scores[...] = lax.dot_general(
            qb[head, at, :], kb[head], (((1,), (1,)), ((), ())), preferred_element_type=F32
        )

    def mix(head, t, scores):
        to = (y + order[t]) % 4
        highest = jnp.max(scores[...], axis=-1, keepdims=True) * EXP_SCALE
        weights = jnp.exp2(scores[...] * EXP_SCALE - highest).astype(BF16)
        total = jnp.dot(weights, vb[head], preferred_element_type=F32)
        mixed = jnp.where(wide_lane < HEAD_DIM, total / total[:, HEAD_DIM : HEAD_DIM + 1], 0.0)
        csend[head, to] = mixed.astype(BF16)

    def attend(head, between):
        slots = (score_a, score_b)
        score(head, 0, slots[0])
        for t in range(4):
            if t < 3:
                score(head, t + 1, slots[(t + 1) % 2])
            mix(head, t, slots[t % 2])
            if t < 3:
                c_copy(head, t).start()
            if t in between:
                between[t]()
        cin[head, y] = csend[head, y]

    def z_place(of_half, of_part):
        return of_half, pl.ds(pl.multiple_of(384 * of_part, 128), 384)

    def z_copy(head, d):
        at_half, at = z_place(half, part)
        return pltpu.make_async_remote_copy(
            src_ref=zsend.at[head, d], dst_ref=ctx.at[head, at_half, :, at],
            send_sem=z_send.at[head, d], recv_sem=z_recv.at[head, d],
            device_id=dev(zl=(zl + d) % 4), device_id_type=MESH,
        )

    def z_wait(head):
        for d in (1, 2, 3):
            source = (zl + 4 - d) % 4
            at_half, at = z_place(source // 2, source % 2)
            ref = ctx.at[head, at_half, :, at]
            pltpu.make_async_remote_copy(
                src_ref=ref, dst_ref=ref, send_sem=z_send.at[head, d], recv_sem=z_recv.at[head, d],
                device_id=dev(zl=partner), device_id_type=MESH,
            ).wait_recv()

    def give_back(head):
        for t in range(3):
            c_wait(head, t)
        for d in (2, 3, 1, 0):
            to = (zl + d) % 4
            at = pl.ds(pl.multiple_of(to * TOK, 16), TOK)
            joined = None
            for s in range(4):
                piece = cin[head, s, at, :].astype(F32)
                wide = jnp.concatenate([piece, jnp.zeros((TOK, 256), F32)], axis=1)
                if s:
                    wide = pltpu.roll(wide, 80 * s, 1)
                joined = wide if joined is None else joined + wide
            if d:
                zsend[head, d] = joined.astype(BF16)
                z_copy(head, d).start()
            else:
                at_half, at = z_place(half, part)
                ctx[head, at_half, :, at] = joined.astype(BF16)

    rows = 2 * TOK

    def project(head):
        @pl.loop(0, 5, unroll=True)
        def _(n):
            at = pl.ds(pl.multiple_of(256 * n, 256), 256)
            made = None
            for p in range(2):
                block = wout[2 * p : 2 * p + 2, :, head, :, at].reshape(320, 256)
                left = ctx[head, :, :, 384 * p : 384 * p + 320].reshape(rows, 320)
                term = jnp.dot(left, block, preferred_element_type=F32)
                made = term if made is None else made + term
            if head == 0:
                mid[:, at] = x_ref[:, :, at].reshape(rows, 256).astype(F32) + made + row_of(out_bias, at)
            else:
                mid[:, at] += made

    unpack(0)
    class_swap(2)
    ring_relay(3, 0)
    attend(0, {1: lambda: ring_end(1, 0), 2: lambda: ring_end(2, 0)})
    ring_relay(1, 1)
    class_swap(3)
    unpack(1)
    attend(1, {1: lambda: class_ring(2)})
    give_back(0)
    class_ring(3)
    give_back(1)
    ring_relay(2, 1)
    ring_end(3, 0)
    ring_end(1, 1)
    sibling_wait(1, 0)
    sibling_wait(1, 1)
    z_wait(0)
    project(0)
    z_wait(1)
    project(1)
    ring_relay(3, 1)
    ring_end(2, 1)

    @pl.loop(0, rows // 48)
    def _(n):
        at = pl.ds(pl.multiple_of(n * 48, 16), 48)
        normed_mlp[at, :] = norm_rows(mid[at, :], mlp_gain, mlp_shift).astype(BF16)

    sibling_wait(2, 0)
    sibling_wait(2, 1)

    @pl.loop(0, 10, unroll=2)
    def _(n):
        at = pl.ds(pl.multiple_of(256 * n, 256), 256)
        block = wup[:, :, :, :, at].reshape(D, 256)
        lifted = jnp.dot(normed_mlp[...], block, preferred_element_type=F32) + row_of(up_bias, at)
        hid[:, at] = (0.5 * lifted * (1.0 + lax.erf(lifted * math.sqrt(0.5)))).astype(BF16)

    ring_end(3, 1)
    sibling_wait(3, 0)
    sibling_wait(3, 1)

    @pl.loop(0, 5, unroll=True)
    def _(n):
        at = pl.ds(pl.multiple_of(256 * n, 256), 256)
        block = wdown[:, :, :, :, at].reshape(FF, 256)
        lowered = jnp.dot(hid[...], block, preferred_element_type=F32)
        result = mid[:, at] + lowered + row_of(down_bias, at)
        o_ref[:, :, at] = result.astype(BF16).reshape(2, TOK, 256)

    for copy in started:
        copy.wait_send()
    to_partner.wait_send()
    to_near.wait_send()

    @pl.when(is_near)
    def _():
        to_far.wait_send()
        onward.wait_send()

    @pl.loop(0, 4)
    def _(slot):
        for head in range(2):
            for r in (1, 2, 3):
                y_copy(r, head, slot).wait_send()

    for head in range(2):
        for t in range(3):
            c_copy(head, t).wait_send()
        for d in (1, 2, 3):
            z_copy(head, d).wait_send()
    first_sent()


def layer(
    tokens, pre_gain, pre_shift, w_qkv, qkv_bias, w_out, out_bias,
    mlp_gain, mlp_shift, w_up, up_bias, w_down, down_bias,
):
    vmem = pl.BlockSpec(memory_space=pltpu.VMEM)
    hbm = pl.BlockSpec(memory_space=pltpu.HBM)
    dma = pltpu.SemaphoreType.DMA
    vectors = (pre_gain, pre_shift, qkv_bias, out_bias, mlp_gain, mlp_shift, up_bias, down_bias)
    return pl.pallas_call(
        kernel,
        out_shape=jax.ShapeDtypeStruct((2, TOK, D), BF16),
        in_specs=[hbm] * 13,
        out_specs=vmem,
        scratch_shapes=[
            pltpu.VMEM((2, TOK, D), BF16),
            *[pltpu.VMEM(vector.shape, F32) for vector in vectors],
            pltpu.VMEM((4, 2, 2, 80, HALF), BF16),
            pltpu.VMEM((4, 2, 2, 80, D), BF16),
            pltpu.VMEM((4, 2, 2, 80, FF), BF16),
            pltpu.VMEM((4, 2, 2, 160, D), BF16),
            pltpu.VMEM((4, TOK, D), BF16),
            pltpu.VMEM((TOK, D), BF16),
            pltpu.VMEM((TOK, HALF), F32),
            pltpu.VMEM((2, 4, 4, TOK, 256), BF16),
            pltpu.VMEM((2, 4, 4, TOK, 256), BF16),
            pltpu.VMEM((2, SEQ, 128), BF16),
            pltpu.VMEM((2, SEQ, 128), BF16),
            pltpu.VMEM((2, SEQ, 128), BF16),
            pltpu.VMEM((4 * TOK, SEQ), F32),
            pltpu.VMEM((4 * TOK, SEQ), F32),
            pltpu.VMEM((2, 4, 4 * TOK, 128), BF16),
            pltpu.VMEM((2, 4, 4 * TOK, 128), BF16),
            pltpu.VMEM((2, 4, TOK, 384), BF16),
            pltpu.VMEM((2, 2, TOK, 768), BF16),
            pltpu.VMEM((2 * TOK, D), F32),
            pltpu.VMEM((2 * TOK, D), BF16),
            pltpu.VMEM((2 * TOK, FF), BF16),
            dma((13,)), dma((4, 21)), dma((4, 21)), dma((4,)), dma((4,)),
            dma((2, 3, 4)), dma((2, 3, 4)), dma((2, 3)), dma((2, 3)), dma((2, 4)), dma((2, 4)),
        ],
        compiler_params=pltpu.CompilerParams(
            collective_id=0, has_side_effects=True, vmem_limit_bytes=67043328
        ),
    )(
        tokens, *vectors,
        w_qkv, w_out, w_up, w_down,
    )


def solution(mesh):
    in_specs = (
        P("dp", "seq", None),
        P(), P(), P("dp", None), P(), P("dp", None), P(), P(), P(), P("dp", None), P(),
        P("dp", None), P(),
    )
    out_specs = P("dp", "seq", None)
    return jax.shard_map(layer, mesh=mesh, in_specs=in_specs, out_specs=out_specs, check_vma=False)
```

```python
import math

import jax
import jax.numpy as jnp
from jax import lax
from jax.experimental import pallas as pl
from jax.experimental.pallas import tpu as pltpu
from jax.sharding import PartitionSpec as P

D = 1280
HEADS = 16
HEAD_DIM = 80
FF = 2560
TOK = 144
SEQ = 2304
HALF = 1920
PAIR = 480
EPSILON = 1e-05
EXP_SCALE = math.log2(math.e) / math.sqrt(HEAD_DIM)

MESH = pl.DeviceIdType.MESH
F32 = jnp.float32
BF16 = jnp.bfloat16

COLS = (HALF, D, FF, D)
LOW = (1024, 640, 1280, 640)
ROWS = (80, 80, 80, 160)
XM, XP, X2L, X2R, ZC, YC, YQ, DC = 0, 1, 2, 3, 8, 9, 10, 13


def kernel(
    x_in, pre_gain_in, pre_shift_in, qkv_bias_in, out_bias_in, mlp_gain_in, mlp_shift_in,
    up_bias_in, down_bias_in,
    wqkv_in, wout_in, wup_in, wdown_in,
    o_ref,
    x_ref, pre_gain, pre_shift, qkv_bias, out_bias, mlp_gain, mlp_shift, up_bias, down_bias,
    wqkv, wout, wup, wdown,
    tok, other, packed, qsend, qin, qb, kb, vb, score_a, score_b, csend, cin, zsend, ctx, mid, normed_mlp, hid,
    load_sem, w_send, w_recv, t_send, t_recv, y_send, y_recv, c_send, c_recv, z_send, z_recv,
):
    dp = lax.axis_index("dp")
    sq = lax.axis_index("seq")
    x, zh, c = dp // 4, (dp // 2) % 2, dp % 2
    zl, y = sq // 4, sq % 4
    half, part = zl // 2, zl % 2

    def dev(x=x, zh=zh, c=c, zl=zl, y=y):
        return ((x * 2 + zh) * 2 + c, zl * 4 + y)

    xr, xl, xo = (x + 1) % 4, (x + 3) % 4, (x + 2) % 4
    ypair = y + 1 - 2 * (y % 2)
    partner = zl + 1 - 2 * part
    near_here = 1 + half
    is_near = zl == near_here
    near_other = 2 - half
    far_other = 3 - 3 * half

    barrier = pltpu.get_barrier_semaphore()
    peers = [dev(x=xr), dev(x=xl), dev(zh=1 - zh), dev(c=1 - c)]
    peers += [dev(zl=(zl + d) % 4) for d in (1, 2, 3)]
    peers += [dev(y=(y + d) % 4) for d in (1, 2, 3)]

    bufs = (wqkv, wout, wup, wdown)
    sources = (
        wqkv_in.at[:, pl.ds(pl.multiple_of(part * HALF, 128), HALF)],
        wout_in,
        wup_in,
        wdown_in,
    )
    loads = [
        pltpu.make_async_copy(sources[i], bufs[i].at[x, zh, c], load_sem.at[i]) for i in range(4)
    ]
    early_in = (x_in, pre_gain_in, pre_shift_in)
    late_in = (qkv_bias_in, out_bias_in, mlp_gain_in, mlp_shift_in, up_bias_in, down_bias_in)
    early_to = (x_ref, pre_gain, pre_shift)
    late_to = (qkv_bias, out_bias, mlp_gain, mlp_shift, up_bias, down_bias)
    early = [
        pltpu.make_async_copy(a, b, load_sem.at[4 + n])
        for n, (a, b) in enumerate(zip(early_in, early_to))
    ]
    late = [
        pltpu.make_async_copy(a, b, load_sem.at[7 + n])
        for n, (a, b) in enumerate(zip(late_in, late_to))
    ]
    for peer in peers:
        pl.semaphore_signal(barrier, inc=1, device_id=peer, device_id_type=MESH)
    for load in (loads[0], *early, *loads[1:], *late):
        load.start()

    started = []

    def region(i, xx, zz, cc, lo=0, size=None):
        size = COLS[i] if size is None else size
        return bufs[i].at[xx, zz, cc, :, pl.ds(lo, size)]

    def w_copy(i, j, ref, target):
        return pltpu.make_async_remote_copy(
            src_ref=ref, dst_ref=ref, send_sem=w_send.at[i, j], recv_sem=w_recv.at[i, j],
            device_id=target, device_id_type=MESH,
        )

    def w_start(i, j, ref, target):
        copy = w_copy(i, j, ref, target)
        copy.start()
        started.append(copy)

    def w_wait(i, j, ref):
        w_copy(i, j, ref, dev(c=1 - c)).wait_recv()

    def side(k):
        return zh if k == 0 else 1 - zh

    def to_sibling(i, k, n, xx):
        w_start(i, DC + 4 * k + n, region(i, xx, side(k), c), dev(c=1 - c))

    def ring_start(i, k):
        mine = region(i, x, side(k), c)
        w_start(i, 4 * k + XM, mine, dev(x=xr))
        w_start(i, 4 * k + XP, mine, dev(x=xl))
        to_sibling(i, k, 0, x)

    def ring_relay(i, k):
        low, high = LOW[i], COLS[i] - LOW[i]
        w_wait(i, 4 * k + XM, region(i, xl, side(k), c))
        w_start(i, 4 * k + X2L, region(i, xl, side(k), c, 0, low), dev(x=xr))
        to_sibling(i, k, 1, xl)
        w_wait(i, 4 * k + XP, region(i, xr, side(k), c))
        w_start(i, 4 * k + X2R, region(i, xr, side(k), c, low, high), dev(x=xl))
        to_sibling(i, k, 2, xr)

    def ring_end(i, k):
        low, high = LOW[i], COLS[i] - LOW[i]
        w_wait(i, 4 * k + X2L, region(i, xo, side(k), c, 0, low))
        w_wait(i, 4 * k + X2R, region(i, xo, side(k), c, low, high))
        to_sibling(i, k, 3, xo)

    def sibling_wait(i, k):
        for n, xx in enumerate((x, xl, xr, xo)):
            w_wait(i, DC + 4 * k + n, region(i, xx, side(k), 1 - c))

    def piece(i, zz, who):
        if i == 1:
            return region(i, x, zz, c, pl.multiple_of(640 * (who % 2), 128), 640)
        if i == 2:
            return region(i, x, zz, c, pl.multiple_of(640 * who, 128), 640)
        down = pl.ds(pl.multiple_of(80 * (who // 2), 16), 80)
        return bufs[i].at[x, zz, c, down, pl.ds(pl.multiple_of(640 * (who % 2), 128), 640)]

    def class_start(i):
        w_start(i, ZC, piece(i, zh, y), dev(zh=1 - zh))

    def class_swap(i):
        mine = piece(i, 1 - zh, y)
        w_wait(i, ZC, mine)
        if i == 1:
            w_start(i, YQ, mine, dev(y=ypair))
        else:
            for r in (2, 1, 3):
                w_start(i, YQ + r - 1, mine, dev(y=(y + r) % 4))

    def class_ring(i):
        if i == 1:
            w_wait(i, YQ, piece(i, 1 - zh, ypair))
        else:
            for r in (1, 2, 3):
                w_wait(i, YQ + r - 1, piece(i, 1 - zh, (y + 4 - r) % 4))
        ring_start(i, 1)

    def uneven(which, j):
        lo, size = (0, LOW[0]) if which == 0 else (LOW[0], COLS[0] - LOW[0])
        if j == ZC:
            return w_copy(0, ZC, region(0, x, zh, c, lo, size), dev(zh=1 - zh))
        return w_copy(0, YC, region(0, x, 1 - zh, c, lo, size), dev(y=ypair))

    def by_parity(act):
        for which in (0, 1):

            @pl.when(y % 2 == which)
            def _():
                act(which)

    def first_start():
        by_parity(lambda which: uneven(which, ZC).start())

    def first_swap():
        def act(which):
            uneven(which, ZC).wait_recv()
            uneven(which, YC).start()

        by_parity(act)

    def first_ring():
        by_parity(lambda which: uneven(1 - which, YC).wait_recv())
        ring_start(0, 1)

    def first_sent():
        def act(which):
            uneven(which, ZC).wait_send()
            uneven(which, YC).wait_send()

        by_parity(act)

    def row_of(ref, at=slice(None)):
        return ref[at].reshape(1, -1)

    def norm_rows(rows, gain, shift):
        average = jnp.mean(rows, axis=-1, keepdims=True)
        centered = rows - average
        spread = jnp.mean(centered * centered, axis=-1, keepdims=True)
        return centered * lax.rsqrt(spread + EPSILON) * row_of(gain) + row_of(shift)

    def norm_image(image, store):
        @pl.loop(0, TOK // 48)
        def _(n):
            at = pl.ds(pl.multiple_of(n * 48, 16), 48)
            rows = x_ref[image, at, :].astype(F32)
            store(at, norm_rows(rows, pre_gain, pre_shift).astype(BF16))

    def store_other(at, value):
        other[at, :] = value

    def store_own(at, value):
        tok[zl, at, :] = value

    def t_copy(src, slot, j, target):
        return pltpu.make_async_remote_copy(
            src_ref=src, dst_ref=tok.at[slot], send_sem=t_send.at[j], recv_sem=t_recv.at[slot],
            device_id=target, device_id_type=MESH,
        )

    for load in early:
        load.wait()
    norm_image(1 - half, store_other)
    norm_image(half, store_own)
    loads[0].wait()
    pl.semaphore_wait(barrier, len(peers))

    first_start()
    ring_start(0, 0)
    to_near = t_copy(other, zl, 1, dev(zl=near_other))
    to_near.start()
    to_far = t_copy(other, zl, 2, dev(zl=far_other))

    @pl.when(is_near)
    def _():
        to_far.start()

    to_partner = t_copy(tok.at[zl], zl, 0, dev(zl=partner))
    to_partner.start()

    for load in (*loads[1:], *late):
        load.wait()
    class_start(1)

    onward = t_copy(tok.at[far_other], far_other, 3, dev(zl=partner))

    def token_wait(slot):
        t_copy(tok.at[slot], slot, 0, dev(zl=partner)).wait_recv()

    first_swap()
    ring_relay(0, 0)
    first_ring()
    ring_end(0, 0)
    ring_relay(0, 1)
    for i in (1, 2, 3):
        ring_start(i, 0)

    @pl.when(is_near)
    def _():
        token_wait(far_other)
        onward.start()

    ring_end(0, 1)
    class_swap(1)
    sibling_wait(0, 0)
    sibling_wait(0, 1)

    def slot_of(j):
        last = jnp.where(j == 2, near_other, far_other)
        return jnp.where(j == 0, zl, jnp.where(j == 1, partner, last))

    def y_copy(r, head, slot):
        to = (y + r) % 4
        return pltpu.make_async_remote_copy(
            src_ref=qsend.at[head, to, slot], dst_ref=qin.at[head, y, slot],
            send_sem=y_send.at[head, r - 1, slot], recv_sem=y_recv.at[head, r - 1, slot],
            device_id=dev(y=to), device_id_type=MESH,
        )

    def y_copy_in(r, head, slot, source):
        return pltpu.make_async_remote_copy(
            src_ref=qin.at[head, source, slot], dst_ref=qin.at[head, source, slot],
            send_sem=y_send.at[head, r - 1, slot], recv_sem=y_recv.at[head, r - 1, slot],
            device_id=dev(y=(y + 1) % 4), device_id_type=MESH,
        )

    def first_projection(j):
        slot = slot_of(j)

        @pl.when((j > 0) & jnp.logical_not((j == 3) & is_near))
        def _():
            token_wait(slot)

        rows = tok[slot]
        bias_at = pl.multiple_of(part * HALF, 128)
        for n in range(3):
            at = slice(640 * n, 640 * n + 640)
            block = wqkv[:, :, :, :, at].reshape(D, 640)
            bias = row_of(qkv_bias, pl.ds(bias_at + 640 * n, 640))
            packed[:, at] = jnp.dot(rows, block, preferred_element_type=F32) + bias
        for head in range(2):
            for to in range(4):
                first = PAIR * to + 240 * head
                start = first // 128 * 128
                wide = packed[:, start : min(start + 384, HALF)]
                shift = first - start
                if shift:
                    wide = pltpu.roll(wide, wide.shape[1] - shift, 1)
                qsend[head, to, slot] = wide[:, :256].astype(BF16)
            qin[head, y, slot] = qsend[head, y, slot]
        for r in (2, 1, 3):
            y_copy(r, 0, slot).start()

    pl.loop(0, 4)(first_projection)

    @pl.loop(0, 4)
    def _(j):
        for r in (2, 1, 3):
            y_copy(r, 1, slot_of(j)).start()

    class_start(2)
    class_start(3)
    for i in (1, 2):
        ring_relay(i, 0)
    class_ring(1)

    lane128 = lax.broadcasted_iota(jnp.int32, (TOK, 128), 1)

    def unpack(head):
        @pl.loop(0, 16)
        def _(n):
            j, r = n // 4, n % 4
            slot = slot_of(j)
            source = (y + 4 - r) % 4

            @pl.when(r > 0)
            def _():
                y_copy_in(r, head, slot, source).wait_recv()

            wide = qin[head, source, slot].astype(F32)
            at = pl.ds(pl.multiple_of((source * 4 + slot) * TOK, 16), TOK)
            keep = lane128 < HEAD_DIM
            keys = pltpu.roll(wide, 256 - 80, 1)[:, :128]
            values = pltpu.roll(wide, 256 - 160, 1)[:, :128]
            ones = jnp.where(lane128 == HEAD_DIM, 1.0, 0.0)
            qb[head, at, :] = jnp.where(keep, wide[:, :128], 0.0).astype(BF16)
            kb[head, at, :] = jnp.where(keep, keys, 0.0).astype(BF16)
            vb[head, at, :] = jnp.where(keep, values, ones).astype(BF16)

    order = (2, 1, 3, 0)

    def c_place(head, source):
        return cin.at[head, pl.ds(pl.multiple_of(source * HEAD_DIM, 16), HEAD_DIM), :]

    def c_copy(head, t):
        to = (y + order[t]) % 4
        return pltpu.make_async_remote_copy(
            src_ref=csend.at[head, to], dst_ref=c_place(head, y),
            send_sem=c_send.at[head, t], recv_sem=c_recv.at[head, t],
            device_id=dev(y=to), device_id_type=MESH,
        )

    def c_wait(head, t):
        source = (y + 4 - order[t]) % 4
        pltpu.make_async_remote_copy(
            src_ref=c_place(head, source), dst_ref=c_place(head, source),
            send_sem=c_send.at[head, t], recv_sem=c_recv.at[head, t],
            device_id=dev(y=(y + 1) % 4), device_id_type=MESH,
        ).wait_recv()

    def score(head, t, scores):
        to = (y + order[t]) % 4
        at = pl.ds(pl.multiple_of(to * 4 * TOK, 16), 4 * TOK)
        scores[...] = lax.dot_general(
            qb[head, at, :], kb[head], (((1,), (1,)), ((), ())), preferred_element_type=F32
        )

    def mix(head, t, scores):
        to = (y + order[t]) % 4
        highest = jnp.max(scores[...], axis=-1, keepdims=True) * EXP_SCALE
        weights = jnp.exp2(scores[...] * EXP_SCALE - highest).astype(BF16)
        total = jnp.dot(weights, vb[head], preferred_element_type=F32)
        mixed = total / total[:, HEAD_DIM : HEAD_DIM + 1]
        tall = jnp.concatenate([mixed, jnp.zeros((64, 128), F32)], axis=0)
        csend[head, to] = tall.T[:HEAD_DIM].astype(BF16)

    def attend(head, between):
        slots = (score_a, score_b)
        score(head, 0, slots[0])
        for t in range(4):
            if t < 3:
                score(head, t + 1, slots[(t + 1) % 2])
            mix(head, t, slots[t % 2])
            if t < 3:
                c_copy(head, t).start()
            if t in between:
                between[t]()
        c_place(head, y)[...] = csend[head, y]

    def z_place(of_half, of_part):
        return of_half, pl.ds(pl.multiple_of(384 * of_part, 128), 384)

    def z_rows(head, to):
        return zsend.at[head, pl.ds(pl.multiple_of(to * TOK, 16), TOK), :]

    def z_copy(head, d):
        at_half, at = z_place(half, part)
        return pltpu.make_async_remote_copy(
            src_ref=z_rows(head, (zl + d) % 4), dst_ref=ctx.at[head, at_half, :, at],
            send_sem=z_send.at[head, d], recv_sem=z_recv.at[head, d],
            device_id=dev(zl=(zl + d) % 4), device_id_type=MESH,
        )

    def z_wait(head):
        for d in (1, 2, 3):
            source = (zl + 4 - d) % 4
            at_half, at = z_place(source // 2, source % 2)
            ref = ctx.at[head, at_half, :, at]
            pltpu.make_async_remote_copy(
                src_ref=ref, dst_ref=ref, send_sem=z_send.at[head, d], recv_sem=z_recv.at[head, d],
                device_id=dev(zl=partner), device_id_type=MESH,
            ).wait_recv()

    def give_back(head):
        for t in range(3):
            c_wait(head, t)
        for n in range(5):
            at = slice(128 * n, 128 * n + 128)
            zsend[head, at, :] = cin[head, :, at].astype(F32).T.astype(BF16)
        for d in (2, 3, 1):
            z_copy(head, d).start()
        at_half, at = z_place(half, part)
        ctx[head, at_half, :, at] = z_rows(head, zl)[...]

    rows = 2 * TOK

    def project(head):
        @pl.loop(0, 5, unroll=True)
        def _(n):
            at = pl.ds(pl.multiple_of(256 * n, 256), 256)
            made = None
            for p in range(2):
                block = wout[2 * p : 2 * p + 2, :, head, :, at].reshape(320, 256)
                left = ctx[head, :, :, 384 * p : 384 * p + 320].reshape(rows, 320)
                term = jnp.dot(left, block, preferred_element_type=F32)
                made = term if made is None else made + term
            if head == 0:
                mid[:, at] = x_ref[:, :, at].reshape(rows, 256).astype(F32) + made + row_of(out_bias, at)
            else:
                mid[:, at] += made

    unpack(0)
    class_swap(2)
    ring_relay(3, 0)
    attend(0, {1: lambda: ring_end(1, 0), 2: lambda: ring_end(2, 0)})
    ring_relay(1, 1)
    class_swap(3)
    unpack(1)
    attend(1, {1: lambda: class_ring(2)})
    give_back(0)
    class_ring(3)
    give_back(1)
    ring_relay(2, 1)
    ring_end(3, 0)
    ring_end(1, 1)
    sibling_wait(1, 0)
    sibling_wait(1, 1)
    z_wait(0)
    project(0)
    z_wait(1)
    project(1)
    ring_relay(3, 1)
    ring_end(2, 1)

    @pl.loop(0, rows // 48)
    def _(n):
        at = pl.ds(pl.multiple_of(n * 48, 16), 48)
        normed_mlp[at, :] = norm_rows(mid[at, :], mlp_gain, mlp_shift).astype(BF16)

    sibling_wait(2, 0)
    sibling_wait(2, 1)

    @pl.loop(0, 10, unroll=2)
    def _(n):
        at = pl.ds(pl.multiple_of(256 * n, 256), 256)
        block = wup[:, :, :, :, at].reshape(D, 256)
        lifted = jnp.dot(normed_mlp[...], block, preferred_element_type=F32) + row_of(up_bias, at)
        hid[:, at] = (0.5 * lifted * (1.0 + lax.erf(lifted * math.sqrt(0.5)))).astype(BF16)

    ring_end(3, 1)
    sibling_wait(3, 0)
    sibling_wait(3, 1)

    @pl.loop(0, 5, unroll=True)
    def _(n):
        at = pl.ds(pl.multiple_of(256 * n, 256), 256)
        block = wdown[:, :, :, :, at].reshape(FF, 256)
        lowered = jnp.dot(hid[...], block, preferred_element_type=F32)
        result = mid[:, at] + lowered + row_of(down_bias, at)
        o_ref[:, :, at] = result.astype(BF16).reshape(2, TOK, 256)

    for copy in started:
        copy.wait_send()
    to_partner.wait_send()
    to_near.wait_send()

    @pl.when(is_near)
    def _():
        to_far.wait_send()
        onward.wait_send()

    @pl.loop(0, 4)
    def _(slot):
        for head in range(2):
            for r in (1, 2, 3):
                y_copy(r, head, slot).wait_send()

    for head in range(2):
        for t in range(3):
            c_copy(head, t).wait_send()
        for d in (1, 2, 3):
            z_copy(head, d).wait_send()
    first_sent()


def layer(
    tokens, pre_gain, pre_shift, w_qkv, qkv_bias, w_out, out_bias,
    mlp_gain, mlp_shift, w_up, up_bias, w_down, down_bias,
):
    vmem = pl.BlockSpec(memory_space=pltpu.VMEM)
    hbm = pl.BlockSpec(memory_space=pltpu.HBM)
    dma = pltpu.SemaphoreType.DMA
    vectors = (pre_gain, pre_shift, qkv_bias, out_bias, mlp_gain, mlp_shift, up_bias, down_bias)
    return pl.pallas_call(
        kernel,
        out_shape=jax.ShapeDtypeStruct((2, TOK, D), BF16),
        in_specs=[hbm] * 13,
        out_specs=vmem,
        scratch_shapes=[
            pltpu.VMEM((2, TOK, D), BF16),
            *[pltpu.VMEM(vector.shape, F32) for vector in vectors],
            pltpu.VMEM((4, 2, 2, 80, HALF), BF16),
            pltpu.VMEM((4, 2, 2, 80, D), BF16),
            pltpu.VMEM((4, 2, 2, 80, FF), BF16),
            pltpu.VMEM((4, 2, 2, 160, D), BF16),
            pltpu.VMEM((4, TOK, D), BF16),
            pltpu.VMEM((TOK, D), BF16),
            pltpu.VMEM((TOK, HALF), F32),
            pltpu.VMEM((2, 4, 4, TOK, 256), BF16),
            pltpu.VMEM((2, 4, 4, TOK, 256), BF16),
            pltpu.VMEM((2, SEQ, 128), BF16),
            pltpu.VMEM((2, SEQ, 128), BF16),
            pltpu.VMEM((2, SEQ, 128), BF16),
            pltpu.VMEM((4 * TOK, SEQ), F32),
            pltpu.VMEM((4 * TOK, SEQ), F32),
            pltpu.VMEM((2, 4, HEAD_DIM, 640), BF16),
            pltpu.VMEM((2, 384, 640), BF16),
            pltpu.VMEM((2, 640, 384), BF16),
            pltpu.VMEM((2, 2, TOK, 768), BF16),
            pltpu.VMEM((2 * TOK, D), F32),
            pltpu.VMEM((2 * TOK, D), BF16),
            pltpu.VMEM((2 * TOK, FF), BF16),
            dma((13,)), dma((4, 21)), dma((4, 21)), dma((4,)), dma((4,)),
            dma((2, 3, 4)), dma((2, 3, 4)), dma((2, 3)), dma((2, 3)), dma((2, 4)), dma((2, 4)),
        ],
        compiler_params=pltpu.CompilerParams(
            collective_id=0, has_side_effects=True, vmem_limit_bytes=67043328
        ),
    )(
        tokens, *vectors,
        w_qkv, w_out, w_up, w_down,
    )


def solution(mesh):
    in_specs = (
        P("dp", "seq", None),
        P(), P(), P("dp", None), P(), P("dp", None), P(), P(), P(), P("dp", None), P(),
        P("dp", None), P(),
    )
    out_specs = P("dp", "seq", None)
    return jax.shard_map(layer, mesh=mesh, in_specs=in_specs, out_specs=out_specs, check_vma=False)
```
